256 devices in a mesh: prow: 32 (over x, z), pcol: 8 (over y, core).
Axes of the slice: x: 4, y: 4, z: 8, core: 2. Of those that a mesh axis runs over, the one named last changes fastest.
Arguments:
- inverse_pool: float32 [12288, 12288], P('prow', 'pcol'), may hold values from -6 to 6
- panel_one: float32 [12288, 512], P(('prow', 'pcol')), may hold values from -0.0625 to 0.0625
- panel_two: float32 [12288, 512], P(('prow', 'pcol')), may hold values from -0.078125 to 0.078125
- upper_two: float32 [512, 512], replicated, may hold values from -0.25 to 0.25
- lower_one: float32 [512, 512], replicated, as said below
- lower_two: float32 [512, 512], replicated, as said below
- list_one: int32 [72], replicated, may hold values from 0 to 95, as said below
- list_two: int32 [48], replicated, may hold values from 0 to 95, as said below
Outputs:
- first_offdiag: float32 [12288, 512], P(('prow', 'pcol'))
- first_diag: float32 [512, 512], replicated
- second_offdiag: float32 [12288, 512], P(('prow', 'pcol'))
- second_coupling: float32 [512, 512], replicated
- second_diag: float32 [512, 512], replicated
The draws below stay inside these ranges and needn't reach their ends.
Inputs may be any that keep to these rules, and one draw needn't show every extreme that they name: `list_one`: distinct block numbers, among them 0, 48 and 95. `list_two`: distinct block numbers, each of which is also in list_one, among them 0, 48 and 95. `lower_one`: lower triangular with a diagonal of 1 to 1.5. `lower_two`: lower triangular with a diagonal of 1 to 1.5.
All inputs are finite; a program needn't handle non-finite values.
Results may differ from the reference program's by a relative error of at most 0.000073.
Values sent between devices are 32-bit elements; how exact they have to be, the bound alone decides.
No kernel may reach another device: no remote copies, remote signals or barrier semaphores. Data moves between devices by JAX's collectives and lax.ppermute only.
A program may use at most 64 MiB of HBM per device.

```python
import jax
import jax.numpy as jnp
from jax import lax

W = 512
BLK = 128
NP = 12288
NBLK = 96
NSEL1 = 72
NSEL2 = 48


def lower_factor(key):
    strict = jax.random.normal(jax.random.fold_in(key, 3), (W, W), jnp.float32) * (0.6 / W ** 0.5)
    diagonal = 1.0 + 0.5 * jax.random.uniform(jax.random.fold_in(key, 4), (W,), jnp.float32)
    return jnp.tril(strict, -1) + jnp.diag(diagonal)


def draw_lower_one(key, part):
    return lower_factor(jax.random.fold_in(key, 21))


def draw_lower_two(key, part):
    return lower_factor(jax.random.fold_in(key, 22))


def ancestor_order(key):
    shuffled = jax.random.permutation(jax.random.fold_in(key, 11), NBLK).astype(jnp.int32)
    blocks = jnp.arange(NBLK, dtype=jnp.int32)
    middle = NP // 2 // BLK
    scores = shuffled + 3
    scores = jnp.where(blocks == 0, 0, scores)
    scores = jnp.where(blocks == middle, 1, scores)
    scores = jnp.where(blocks == NBLK - 1, 2, scores)
    return jnp.argsort(scores, stable=True).astype(jnp.int32)


def draw_list_one(key, part):
    chosen = ancestor_order(key)[:NSEL1]
    return jax.random.permutation(jax.random.fold_in(key, 13), chosen).astype(jnp.int32)


def draw_list_two(key, part):
    chosen = ancestor_order(key)[:NSEL2]
    return jax.random.permutation(jax.random.fold_in(key, 12), chosen).astype(jnp.int32)


def block_levels(rng, shape, split, low, top_value):
    def one(dim, parts):
        draws = jax.random.uniform(jax.random.fold_in(jax.random.fold_in(rng, 6), dim), (parts,), jnp.float32, low / len(split), top_value / len(split))
        return jnp.repeat(jnp.exp(draws), shape[dim] // parts).reshape((-1,) + (1,) * (len(shape) - dim - 1))

    factor_of = one(*split[0])
    for cut in split[1:]:
        factor_of = factor_of * one(*cut)
    return factor_of


def centred(own_key, extent, deviation, reach, shards=(), kind=jnp.bfloat16):
    loudness = block_levels(own_key, extent, shards, -0.22, 0.18) if shards else 1.0
    drawn = jax.random.normal(own_key, extent, jnp.float32) * deviation * loudness
    return jnp.minimum(jnp.maximum(drawn, -reach), reach).astype(kind)


def setup_inputs(seed: int = 0) -> dict:
    streams_of = jax.random.split(jax.random.key(seed), 9)
    inverse_pool = centred(streams_of[0], (NP, NP), 1.0, 6.0, ((0, 32), (1, 8)), jnp.float32)
    panel_one = centred(streams_of[1], (NP, W), (NSEL1 * BLK) ** -0.5, 0.0625, ((0, 256),), jnp.float32)
    panel_two = centred(streams_of[2], (NP, W), (NSEL2 * BLK) ** -0.5, 0.078125, ((0, 256),), jnp.float32)
    upper_two = centred(streams_of[3], (W, W), W ** -0.5, 0.25, (), jnp.float32)
    lower_one = draw_lower_one(jax.random.fold_in(streams_of[8], 71), 0)
    lower_two = draw_lower_two(jax.random.fold_in(streams_of[8], 71), 0)
    list_one = draw_list_one(jax.random.fold_in(streams_of[8], 71), 0)
    list_two = draw_list_two(jax.random.fold_in(streams_of[8], 71), 0)
    return dict(inverse_pool=inverse_pool, panel_one=panel_one, panel_two=panel_two, upper_two=upper_two, lower_one=lower_one, lower_two=lower_two, list_one=list_one, list_two=list_two)


def product(left, right):
    return jnp.dot(left, right, precision=lax.Precision.HIGHEST, preferred_element_type=jnp.float32)


def transposed_product(left, right):
    return lax.dot_general(left, right, (((0,), (0,)), ((), ())), precision=lax.Precision.HIGHEST, preferred_element_type=jnp.float32)


def live_rows(listing):
    blocks = jnp.arange(NP, dtype=jnp.int32) // BLK
    hits = jnp.any(blocks[:, None] == listing[None, :].astype(jnp.int32), axis=1)
    return jnp.where(hits, 1.0, 0.0).astype(jnp.float32)[:, None]


def reference(inverse_pool, panel_one, panel_two, upper_two, lower_one, lower_two, list_one, list_two):
    live_one = live_rows(list_one)
    live_two = live_rows(list_two)
    masked_one = live_one * panel_one
    masked_two = live_two * panel_two
    first_offdiag = -live_one * product(inverse_pool, masked_one)
    first_diag = transposed_product(lower_one, lower_one) - transposed_product(masked_one, first_offdiag)
    second_offdiag = -live_two * (product(first_offdiag, upper_two) + product(inverse_pool, masked_two))
    second_coupling = -(product(first_diag, upper_two) + transposed_product(first_offdiag, masked_two))
    second_diag = transposed_product(lower_two, lower_two) - transposed_product(upper_two, second_coupling) - transposed_product(masked_two, second_offdiag)
    return first_offdiag, first_diag, second_offdiag, second_coupling, second_diag
```

```python
import functools

import jax
import jax.numpy as jnp
from jax import lax
from jax.experimental import pallas as pl
from jax.experimental.pallas import tpu as pltpu
from jax.sharding import Mesh
from jax.sharding import PartitionSpec as P


BLK = 128
SIZES = {"x": 4, "z": 8, "y": 4, "k": 2}
ALL = ("x", "z", "y", "k")
F32 = jnp.float32
BF16 = jnp.bfloat16


def call(body, out_shapes, *args, scratch=(), smem=0):
    whole = pl.BlockSpec(memory_space=pltpu.VMEM)
    scalars = pl.BlockSpec(memory_space=pltpu.SMEM)
    return pl.pallas_call(
        body,
        out_shape=out_shapes,
        in_specs=[scalars] * smem + [whole] * (len(args) - smem),
        out_specs=jax.tree.map(lambda _: whole, out_shapes),
        scratch_shapes=list(scratch),
    )(*args)


def arr(*shape, dtype=F32):
    return jax.ShapeDtypeStruct(shape, dtype)


def halves(v):
    hi = v.astype(BF16)
    return hi, (v - hi.astype(F32)).astype(BF16)


def dot3(a_hi, a_lo, b_hi, b_lo, dims):
    def one(a, b):
        return lax.dot_general(a, b, (dims, ((), ())), preferred_element_type=F32)

    return one(a_hi, b_hi) + (one(a_hi, b_lo) + one(a_lo, b_hi))


def shifted(v, axis, by):
    n = SIZES[axis]
    return lax.ppermute(v, axis, [(i, (i + by) % n) for i in range(n)])


def spread(v, axis):
    return [v] + [shifted(v, axis, d) for d in range(1, SIZES[axis])]


def exchanged(pieces, axis):
    return [pieces[0]] + [shifted(pieces[d], axis, d) for d in range(1, SIZES[axis])]


def place(axis, d, step):
    n = SIZES[axis]
    return pl.multiple_of(lax.rem(lax.axis_index(axis) + (n + d) % n, n) * step, step)


def merged_rows(pieces, axis, cuts=1):
    n = SIZES[axis]
    rows, cols = pieces[0].shape

    def body(*refs):
        for d in range(n):
            refs[n][pl.ds(place(axis, -d, rows), rows), :] = refs[d][...]

    return call(body, arr(n * rows, cols), *pieces)


def merged_cols(pieces, axis):
    n = SIZES[axis]
    rows, cols = pieces[0].shape

    def body(*refs):
        for d in range(n):
            refs[n][:, pl.ds(place(axis, -d, cols), cols)] = refs[d][...]

    return call(body, arr(rows, n * cols), *pieces)


def summed_split(terms, axis, dim):
    n = SIZES[axis]
    rows, cols = terms[0].shape
    m = len(terms)
    part = (rows // n, cols) if dim == 0 else (rows, cols // n)

    def body(*refs):
        total = refs[-1]
        v = refs[0][...]
        for r in refs[1:m]:
            v = v + r[...]
        total[...] = v
        for d in range(n):
            at = pl.ds(place(axis, d, part[dim]), part[dim])
            refs[m + d][...] = total[at, :] if dim == 0 else total[:, at]

    return call(body, [arr(*part)] * n, *terms, scratch=[pltpu.VMEM((rows, cols), F32)])


def masks(list_one, list_two, panel_one, panel_two):
    rows, cols = panel_one.shape

    def body(one_list, two_list, one, two, m1, m2, both, keep1, keep2):
        index = lax.axis_index("x")
        for axis in ("z", "y", "k"):
            index = index * SIZES[axis] + lax.axis_index(axis)
        first = index * rows
        block = first // BLK
        edge = (block + 1) * BLK - first
        row = lax.broadcasted_iota(jnp.int32, (rows, BLK), 0)
        for listing, panel, out, keep, at in ((one_list, one, m1, keep1, 0), (two_list, two, m2, keep2, cols)):
            near = jnp.int32(0)
            far = jnp.int32(0)
            for i in range(listing.shape[0]):
                near = near + (listing[i] == block).astype(jnp.int32)
                far = far + (listing[i] == block + 1).astype(jnp.int32)
            hits = jnp.where(row < edge, near, far)
            live = jnp.where(hits > 0, 1.0, 0.0).astype(F32)
            keep[...] = live
            for c in range(0, cols, BLK):
                v = live * panel[:, c : c + BLK]
                out[:, c : c + BLK] = v
                both[:, at + c : at + c + BLK] = v

    shapes = [arr(rows, cols), arr(rows, cols), arr(rows, 2 * cols), arr(rows, BLK), arr(rows, BLK)]
    return call(body, shapes, list_one, list_two, panel_one, panel_two, smem=2)


def split_tile(tile, span):
    rows, cols = tile.shape
    n = rows // (2 * span)

    def body(a, hi, lo):
        k = lax.axis_index("k")
        for half, core in ((0, k), (1, 1 - k)):
            for b in range(n):
                v = a[pl.ds(pl.multiple_of((2 * b + core) * span, span), span), :]
                h, l = halves(v)
                at = half * (rows // 2) + b * span
                hi[at : at + span, :] = h
                lo[at : at + span, :] = l

    return call(body, [arr(rows, cols, dtype=BF16)] * 2, tile)


def multiply(tile_hi, tile_lo, chunks, axis):
    rows, depth = tile_hi.shape
    step, cols = chunks[0][0].shape
    m = len(chunks)

    def body(*refs):
        hi, lo = refs[0], refs[1]
        keep, send, b_hi, b_lo = refs[2 + m :]
        for ref, (_, d) in zip(refs[2 : 2 + m], chunks):
            at = pl.ds(place(axis, d, step), step)
            h, l = halves(ref[...])
            b_hi[at, :] = h
            b_lo[at, :] = l
        v = dot3(hi[...], lo[...], b_hi[...], b_lo[...], ((1,), (0,)))
        keep[...] = v[: rows // 2]
        send[...] = v[rows // 2 :]

    return call(
        body,
        [arr(rows // 2, cols)] * 2,
        tile_hi,
        tile_lo,
        *[c for c, _ in chunks],
        scratch=[pltpu.VMEM((depth, cols), BF16)] * 2,
    )


def contract(terms, masked, width, offset):
    rows, cols = terms[0].shape
    n = SIZES["y"]
    m = len(terms)

    def body(*refs):
        v = refs[0][...]
        for r in refs[1:m]:
            v = v + r[...]
        left, keep, send = refs[m], refs[m + 1], refs[m + 2]
        pieces, total = refs[m + 3 : m + 3 + n], refs[-1]
        total[...] = v
        v_hi, v_lo = halves(v)
        k = lax.axis_index("k")
        for out, core in ((send, 1 - k), (keep, k)):
            at = pl.multiple_of(offset + core * width, width)
            l_hi, l_lo = halves(left[:, pl.ds(at, width)])
            out[...] = dot3(l_hi, l_lo, v_hi, v_lo, ((0,), (0,)))
        for d in range(n):
            pieces[d][...] = total[pl.ds(place("y", d, rows // n), rows // n), :]

    shapes = [arr(width, cols)] * 2 + [arr(rows // n, cols)] * n
    out = call(body, shapes, *terms, masked, scratch=[pltpu.VMEM((rows, cols), F32)])
    return out[0], out[1], out[2:]


def over_column(keep, send, masked, width, offset):
    arrived = lax.ppermute(send, "k", [(0, 1), (1, 0)])
    pieces = summed_split([keep, arrived], "y", 1)
    return contract(exchanged(pieces, "y"), masked, width, offset)


def cut_rows(v, cuts):
    step = v.shape[0] // cuts
    return [v[i * step : (i + 1) * step] for i in range(cuts)]


def everywhere(keep, send):
    arrived = lax.ppermute(send, "k", [(0, 1), (1, 0)])
    terms = exchanged(summed_split([keep, arrived], "x", 0), "x")
    terms = exchanged(summed_split(terms, "z", 0), "z")
    own = functools.reduce(lambda a, b: a + b, terms)
    strip = merged_rows(spread(own, "z"), "z")
    top, bottom = cut_rows(strip, 2)
    half = top.shape[0]
    tops = spread(merged_rows(spread(top, "x"), "x"), "y")
    bottoms = spread(merged_cols(spread(bottom, "y"), "y"), "x")
    wide = bottoms[0].shape[1]

    def body(*refs):
        out = refs[8]
        for d in range(4):
            columns = pl.ds(place("y", -d, BLK), BLK)
            for x in range(4):
                out[2 * half * x : 2 * half * x + half, columns] = refs[d][half * x : half * (x + 1), :]
            out[pl.ds(place("x", -d, 2 * half) + half, half), :] = refs[4 + d][...]

    mine = call(body, arr(8 * half, wide), *tops, *bottoms)
    return mine, lax.ppermute(mine, "k", [(0, 1), (1, 0)])


def product(left, right):
    return jnp.dot(left, right, precision=lax.Precision.HIGHEST, preferred_element_type=F32)


def transposed_product(left, right):
    return lax.dot_general(
        left, right, (((0,), (0,)), ((), ())), precision=lax.Precision.HIGHEST, preferred_element_type=F32
    )


def owners(place_of):
    pairs = []
    for n in range(256):
        column, j = n // 32, n % 32
        x, z = place_of(j)
        pairs.append((n, (x * 8 + z) * 8 + column))
    return pairs


def local(inverse_pool, panel_one, panel_two, upper_two, lower_one, lower_two, list_one, list_two):
    span = panel_one.shape[0]
    width = panel_one.shape[1]
    masked_one, masked_two, masked_both, keep_one, keep_two = masks(list_one, list_two, panel_one, panel_two)
    tile_hi, tile_lo = split_tile(inverse_pool, span)

    moved_one = lax.ppermute(masked_one, ALL, owners(lambda j: (j % 4, j // 4)))
    moved_two = lax.ppermute(masked_two, ALL, owners(lambda j: (j // 8, j % 8)))
    beside = merged_rows(spread(masked_both, "y"), "y")

    strip = merged_rows(spread(moved_one, "x"), "x")
    chunks = [(strip, 0)]
    up = down = strip
    for s in range(1, 5):
        up = shifted(up, "z", 1)
        chunks.append((up, -s))
        if s < 4:
            down = shifted(down, "z", -1)
            chunks.append((down, s))

    line = [None] * 8
    line[0] = up = down = moved_two
    for s in range(1, 5):
        up = shifted(up, "z", 1)
        line[s] = up
        if s < 4:
            down = shifted(down, "z", -1)
            line[8 - s] = down
    block = merged_rows(line, "z")
    blocks = [(v, -d) for d, v in enumerate(spread(block, "x"))]

    keep, send = multiply(tile_hi, tile_lo, chunks, "z")
    one_keep, one_send, one_rows = over_column(keep, send, beside, width, 0)
    keep, send = multiply(tile_hi, tile_lo, blocks, "x")
    two_keep, two_send, two_rows = over_column(keep, send, beside, width // 2, width)

    product_one = merged_cols(exchanged(one_rows, "y"), "y")
    product_two = merged_cols(exchanged(two_rows, "y"), "y")
    first_offdiag = -keep_one[:, :1] * product_one
    second_offdiag = -keep_two[:, :1] * (product(first_offdiag, upper_two) + product_two)

    core = lax.axis_index("k")
    mine, other = everywhere(one_keep, one_send)
    first_terms = jnp.where(core == 0, mine, other)
    coupling_terms = jnp.where(core == 0, other, mine)
    first_diag = transposed_product(lower_one, lower_one) + first_terms
    second_coupling = coupling_terms.T - product(first_diag, upper_two)
    rest = (
        transposed_product(lower_two, lower_two)
        - transposed_product(upper_two, second_coupling)
        - product(coupling_terms, upper_two)
    )
    mine, other = everywhere(two_keep, two_send)
    last_terms = jnp.concatenate([jnp.where(core == 0, mine, other), jnp.where(core == 0, other, mine)])
    second_diag = rest + last_terms
    return (first_offdiag, first_diag, second_offdiag, second_coupling, second_diag)


def solution(mesh):
    finer = Mesh(mesh.devices.reshape(4, 8, 4, 2), ALL)
    rows, columns = ("x", "z"), ("y", "k")
    placed = (P(rows, columns), P(ALL, None), P(ALL, None), P(), P(), P(), P(), P())
    return jax.shard_map(
        local,
        mesh=finer,
        in_specs=placed,
        out_specs=(P(ALL, None), P(), P(ALL, None), P(), P()),
        check_vma=False,
    )
```

```python
import jax
import jax.numpy as jnp
from jax import lax
from jax.experimental import pallas as pl
from jax.experimental.pallas import tpu as pltpu
from jax.sharding import Mesh
from jax.sharding import PartitionSpec as P


BLK = 128
SIZES = {"x": 4, "z": 8, "y": 4, "k": 2}
ALL = ("x", "z", "y", "k")
F32 = jnp.float32
BF16 = jnp.bfloat16


def call(body, out_shapes, *args, scratch=()):
    whole = pl.BlockSpec(memory_space=pltpu.VMEM)
    return pl.pallas_call(
        body,
        out_shape=out_shapes,
        in_specs=[whole] * len(args),
        out_specs=jax.tree.map(lambda _: whole, out_shapes),
        scratch_shapes=list(scratch),
    )(*args)


def arr(*shape, dtype=F32):
    return jax.ShapeDtypeStruct(shape, dtype)


def halves(v):
    hi = v.astype(BF16)
    return hi, (v - hi.astype(F32)).astype(BF16)


def dot3(a, b, dims):
    def one(l, r):
        return lax.dot_general(l, r, (dims, ((), ())), preferred_element_type=F32)

    return one(a[0], b[0]) + (one(a[0], b[1]) + one(a[1], b[0]))


def shifted(v, axis, by):
    n = SIZES[axis]
    return lax.ppermute(v, axis, [(i, (i + by) % n) for i in range(n)])


def crossed(v, axis, mask):
    return lax.ppermute(v, axis, [(i, i ^ mask) for i in range(SIZES[axis])])


def traded(v, axis):
    return lax.all_to_all(v, axis, split_axis=0, concat_axis=0, tiled=True)


def spread(v, axis):
    return [v] + [shifted(v, axis, d) for d in range(1, SIZES[axis])]


def place(axis, d, step):
    n = SIZES[axis]
    return pl.multiple_of(lax.rem(lax.axis_index(axis) + (n + d) % n, n) * step, step)


def masks(list_one, list_two, panel_one, panel_two):
    rows, cols = panel_one.shape

    def body(one_list, two_list, one, two, both, keep1, keep2):
        index = lax.axis_index("x")
        for axis in ("z", "y", "k"):
            index = index * SIZES[axis] + lax.axis_index(axis)
        for listing, panel, keep, at in ((one_list, one, keep1, 0), (two_list, two, keep2, cols)):
            row = lax.broadcasted_iota(jnp.int32, (rows, listing.shape[1]), 0) + index * rows
            hits = jnp.where(lax.shift_right_logical(row, 7) == listing[...], 1.0, 0.0).astype(F32)
            live = jnp.max(hits, axis=1, keepdims=True)
            keep[...] = jnp.broadcast_to(live, (rows, BLK))
            both[:, at : at + cols] = live * panel[...]

    shapes = [arr(rows, 2 * cols), arr(rows, BLK), arr(rows, BLK)]
    return call(body, shapes, list_one[None], list_two[None], panel_one, panel_two)


def split_tile(tile, span):
    rows, cols = tile.shape
    n = rows // (2 * span)

    def body(a, hi, lo):
        k = lax.axis_index("k")
        for half, core in ((0, k), (1, 1 - k)):
            for b in range(n):
                v = a[pl.ds(pl.multiple_of((2 * b + core) * span, span), span), :]
                h, l = halves(v)
                at = half * (rows // 2) + b * span
                hi[at : at + span, :] = h
                lo[at : at + span, :] = l

    return call(body, [arr(rows, cols, dtype=BF16)] * 2, tile)


def stacked(pieces, axis, cuts):
    n = SIZES[axis]
    rows, cols = pieces[0].shape
    width = cols // cuts

    def body(*refs):
        for d in range(n):
            for c in range(cuts):
                at = pl.ds(place(axis, -d, rows), rows)
                refs[n + c][at, :] = refs[d][:, c * width : (c + 1) * width]

    return call(body, [arr(n * rows, width)] * cuts, *pieces)


def multiply(tile_hi, tile_lo, chunks, span):
    rows, depth = tile_hi.shape
    cols = chunks[0][0].shape[1]
    m = len(chunks)
    wide = 256

    def body(*refs):
        hi, lo = refs[0], refs[1]
        keep, send, b_hi, b_lo = refs[2 + m :]
        turn = lax.axis_index("z") + 18 - 4 * lax.axis_index("k")
        for ref, (_, d) in zip(refs[2 : 2 + m], chunks):
            order = lax.rem(turn + d, 8)
            first = (lax.shift_right_logical(order, 1) * 8 + lax.rem(order, 2)) * span
            for x in range(4):
                h, l = halves(ref[x * span : (x + 1) * span, :])
                at = pl.ds(pl.multiple_of(first + 2 * x * span, span), span)
                b_hi[at, :] = h
                b_lo[at, :] = l

        def step(i, carry):
            at = pl.ds(pl.multiple_of(i * wide, wide), wide)
            v = dot3((hi[...], lo[...]), (b_hi[:, at], b_lo[:, at]), ((1,), (0,)))
            keep[:, at] = v[: rows // 2]
            send[:, at] = v[rows // 2 :]
            return carry

        lax.fori_loop(0, cols // wide, step, 0)

    return call(
        body,
        [arr(rows // 2, cols)] * 2,
        tile_hi,
        tile_lo,
        *[c for c, _ in chunks],
        scratch=[pltpu.VMEM((depth, cols), BF16)] * 2,
    )


def by_column(keep_one, came_one, keep_two, came_two):
    rows, cols = keep_one.shape
    n = cols // BLK

    def body(k1, c1, k2, c2, out):
        for i in range(n):
            at = slice(i * BLK, (i + 1) * BLK)
            out[i, :, :BLK] = k1[:, at] + c1[:, at]
            out[i, :, BLK:] = k2[:, at] + c2[:, at]

    return call(body, arr(n, rows, 2 * BLK), keep_one, came_one, keep_two, came_two)


def contract(parts, beside):
    n, rows, cols = parts.shape
    width = beside.shape[1] // 2
    half = 3 * width // 2

    def body(ins, left, total, keep, send, terms):
        v = ins[0]
        for i in range(1, n):
            v = v + ins[i]
        total[...] = v
        one = halves(v[:, :BLK])
        two = halves(v[:, BLK:])
        terms[: 2 * width, :] = dot3(halves(left[...]), one, ((0,), (0,)))
        terms[2 * width :, :] = dot3(halves(left[:, width:]), two, ((0,), (0,)))
        k = lax.axis_index("k")
        keep[...] = terms[pl.ds(pl.multiple_of(k * half, half), half), :]
        send[...] = terms[pl.ds(pl.multiple_of((1 - k) * half, half), half), :]

    shapes = [arr(rows, cols)] + [arr(half, BLK)] * 2
    return call(body, shapes, parts, beside, scratch=[pltpu.VMEM((2 * half, BLK), F32)])


def finish(mine, other, gram_one, gram_two, upper):
    n, rows, cols = mine.shape
    side = upper.shape[0]
    half = rows * 4

    def body(own, far, g1, g2, u_ref, d1_ref, c_ref, d2_ref, terms):
        k = lax.axis_index("k")
        for ref, core in ((own, k), (far, 1 - k)):
            for x in range(4):
                at = pl.ds(pl.multiple_of(core * half + x * rows, rows), rows)
                for y in range(4):
                    terms[at, y * cols : (y + 1) * cols] = ref[4 * x + y]
        u = halves(u_ref[...])
        first = g1[...] + terms[:side, :]
        d1_ref[...] = first
        cross = terms[side : 2 * side, :]
        coupling = cross.T - dot3(halves(first), u, ((1,), (0,)))
        c_ref[...] = coupling
        d2_ref[...] = (
            g2[...]
            + terms[2 * side :, :]
            - dot3(halves(cross), u, ((1,), (0,)))
            - dot3(u, halves(coupling), ((0,), (0,)))
        )

    return call(
        body,
        [arr(side, side)] * 3,
        mine,
        other,
        gram_one,
        gram_two,
        upper,
        scratch=[pltpu.VMEM((2 * half, side), F32)],
    )


def product(left, right):
    return jnp.dot(left, right, precision=lax.Precision.HIGHEST, preferred_element_type=F32)


def gram(lower):
    return lax.dot_general(
        lower, lower, (((0,), (0,)), ((), ())), precision=lax.Precision.HIGHEST, preferred_element_type=F32
    )


def owners():
    pairs = []
    for n in range(256):
        column, j = n // 32, n % 32
        order = 2 * (j // 8) + j % 2
        x = (j % 8) // 2
        z = (order - 2 + 4 * (column % 2)) % 8
        pairs.append((n, (x * 8 + z) * 8 + column))
    return pairs


def local(inverse_pool, panel_one, panel_two, upper_two, lower_one, lower_two, list_one, list_two):
    span, width = panel_one.shape
    both, keep_one, keep_two = masks(list_one, list_two, panel_one, panel_two)
    moved = lax.ppermute(both, ALL, owners())
    tile_hi, tile_lo = split_tile(inverse_pool, span)

    streams = [[(s, 0)] for s in stacked(spread(moved, "x"), "x", 2)]
    ups = [s[0][0] for s in streams]
    downs = list(ups)
    for s in range(1, 5):
        for i in range(2):
            ups[i] = shifted(ups[i], "z", 1)
            streams[i].append((ups[i], -s))
            if s < 4:
                downs[i] = shifted(downs[i], "z", -1)
                streams[i].append((downs[i], s))

    (beside,) = stacked(spread(both, "y"), "y", 1)
    keep1, send1 = multiply(tile_hi, tile_lo, streams[0], span)
    came1 = crossed(send1, "k", 1)
    keep2, send2 = multiply(tile_hi, tile_lo, streams[1], span)
    came2 = crossed(send2, "k", 1)
    parts = traded(by_column(keep1, came1, keep2, came2), "y")
    total, keep, send = contract(parts, beside)

    terms = keep + crossed(send, "k", 1)
    terms = jnp.sum(traded(terms.reshape(4, -1, BLK), "x"), axis=0)
    for mask in (1, 2, 4):
        terms = terms + crossed(terms, "z", mask)
    mine = traded(jnp.broadcast_to(terms, (16, *terms.shape)), ("x", "y"))
    other = crossed(mine, "k", 1)
    first_diag, second_coupling, second_diag = finish(mine, other, gram(lower_one), gram(lower_two), upper_two)

    lines = traded(total.reshape(4, span, 2 * BLK), "y")
    product_one = jnp.swapaxes(lines[:, :, :BLK], 0, 1).reshape(span, width)
    product_two = jnp.swapaxes(lines[:, :, BLK:], 0, 1).reshape(span, width)
    first_offdiag = -keep_one[:, :1] * product_one
    second_offdiag = -keep_two[:, :1] * (product(first_offdiag, upper_two) + product_two)
    return (first_offdiag, first_diag, second_offdiag, second_coupling, second_diag)


def solution(mesh):
    finer = Mesh(mesh.devices.reshape(4, 8, 4, 2), ALL)
    rows, columns = ("x", "z"), ("y", "k")
    placed = (P(rows, columns), P(ALL, None), P(ALL, None), P(), P(), P(), P(), P())
    return jax.shard_map(
        local,
        mesh=finer,
        in_specs=placed,
        out_specs=(P(ALL, None), P(), P(ALL, None), P(), P()),
        check_vma=False,
    )
```

```python
import jax
import jax.numpy as jnp
from jax import lax
from jax.experimental import pallas as pl
from jax.experimental.pallas import tpu as pltpu
from jax.sharding import Mesh
from jax.sharding import PartitionSpec as P


BLK = 128
SIZES = {"x": 4, "z": 8, "y": 4, "k": 2}
ALL = ("x", "z", "y", "k")
F32 = jnp.float32
BF16 = jnp.bfloat16


def call(body, out_shapes, *args, scratch=()):
    whole = pl.BlockSpec(memory_space=pltpu.VMEM)
    return pl.pallas_call(
        body,
        out_shape=out_shapes,
        in_specs=[whole] * len(args),
        out_specs=jax.tree.map(lambda _: whole, out_shapes),
        scratch_shapes=list(scratch),
    )(*args)


def arr(*shape, dtype=F32):
    return jax.ShapeDtypeStruct(shape, dtype)


def halves(v):
    hi = v.astype(BF16)
    return hi, (v - hi.astype(F32)).astype(BF16)


def dot3(a, b, dims):
    def one(l, r):
        return lax.dot_general(l, r, (dims, ((), ())), preferred_element_type=F32)

    return one(a[0], b[0]) + (one(a[0], b[1]) + one(a[1], b[0]))


def shifted(v, axis, by):
    n = SIZES[axis]
    return lax.ppermute(v, axis, [(i, (i + by) % n) for i in range(n)])


def crossed(v, axis, mask):
    return lax.ppermute(v, axis, [(i, i ^ mask) for i in range(SIZES[axis])])


def traded(v, axis):
    return lax.all_to_all(v, axis, split_axis=0, concat_axis=0, tiled=True)


def spread(v, axis):
    return [v] + [shifted(v, axis, d) for d in range(1, SIZES[axis])]


def place(axis, d, step):
    n = SIZES[axis]
    return pl.multiple_of(lax.rem(lax.axis_index(axis) + (n + d) % n, n) * step, step)


def masks(list_one, list_two, panel_one, panel_two):
    rows, cols = panel_one.shape

    def body(one_list, two_list, one, two, both, out1, out2, keep1, keep2):
        index = lax.axis_index("x")
        for axis in ("z", "y", "k"):
            index = index * SIZES[axis] + lax.axis_index(axis)
        for listing, panel, out, keep, at in ((one_list, one, out1, keep1, 0), (two_list, two, out2, keep2, cols)):
            row = lax.broadcasted_iota(jnp.int32, (rows, listing.shape[1]), 0) + index * rows
            hits = jnp.where(lax.shift_right_logical(row, 7) == listing[...], 1.0, 0.0).astype(F32)
            live = jnp.max(hits, axis=1, keepdims=True)
            keep[...] = jnp.broadcast_to(live, (rows, BLK))
            v = live * panel[...]
            out[...] = v
            both[:, at : at + cols] = v

    shapes = [arr(rows, 2 * cols)] + [arr(rows, cols)] * 2 + [arr(rows, BLK)] * 2
    return call(body, shapes, list_one[None], list_two[None], panel_one, panel_two)


def split_tile(tile, span):
    rows, cols = tile.shape
    n = rows // (2 * span)

    def body(a, hi, lo):
        k = lax.axis_index("k")
        for half, core in ((0, k), (1, 1 - k)):
            for b in range(n):
                v = a[pl.ds(pl.multiple_of((2 * b + core) * span, span), span), :]
                h, l = halves(v)
                at = half * (rows // 2) + b * span
                hi[at : at + span, :] = h
                lo[at : at + span, :] = l

    return call(body, [arr(rows, cols, dtype=BF16)] * 2, tile)


def stacked(pieces, axis, cuts):
    n = SIZES[axis]
    rows, cols = pieces[0].shape
    width = cols // cuts

    def body(*refs):
        for d in range(n):
            for c in range(cuts):
                at = pl.ds(place(axis, -d, rows), rows)
                refs[n + c][at, :] = refs[d][:, c * width : (c + 1) * width]

    return call(body, [arr(n * rows, width)] * cuts, *pieces)


def stacked_halves(pieces, axis):
    n = SIZES[axis]
    rows, cols = pieces[0].shape

    def body(*refs):
        whole = refs[-1]
        for d in range(n):
            whole[pl.ds(place(axis, -d, rows), rows), :] = refs[d][...]
        refs[n][...] = whole[: n * rows // 2]
        refs[n + 1][...] = whole[n * rows // 2 :]

    return call(body, [arr(n * rows // 2, cols)] * 2, *pieces, scratch=[pltpu.VMEM((n * rows, cols), F32)])


def spot(x, z):
    order = lax.rem(z + 10 - 4 * lax.axis_index("k"), 8)
    turn = lax.rem(x + 4 - lax.axis_index("y"), 4)
    side = jnp.where(turn == 0, 1, jnp.where(turn == 1, 4, jnp.where(turn == 2, 0, 5)))
    return lax.shift_right_logical(order, 1) * 8 + lax.rem(order, 2) * 2 + side


def multiply(tile_hi, tile_lo, chunks, cols, span):
    rows, depth = tile_hi.shape
    m = len(chunks)
    wide = 256

    def body(*refs):
        hi, lo = refs[0], refs[1]
        keep, send, b_hi, b_lo = refs[2 + m :]
        for ref, (_, column, at_of) in zip(refs[2 : 2 + m], chunks):
            for b in range(ref.shape[0] // span):
                h, l = halves(ref[b * span : (b + 1) * span, :])
                at = pl.ds(pl.multiple_of(spot(*at_of(b)) * span, span), span)
                b_hi[at, column : column + ref.shape[1]] = h
                b_lo[at, column : column + ref.shape[1]] = l

        def step(i, carry):
            at = pl.ds(pl.multiple_of(i * wide, wide), wide)
            v = dot3((hi[...], lo[...]), (b_hi[:, at], b_lo[:, at]), ((1,), (0,)))
            keep[:, at] = v[: rows // 2]
            send[:, at] = v[rows // 2 :]
            return carry

        lax.fori_loop(0, cols // wide, step, 0)

    return call(
        body,
        [arr(rows // 2, cols)] * 2,
        tile_hi,
        tile_lo,
        *[c[0] for c in chunks],
        scratch=[pltpu.VMEM((depth, cols), BF16)] * 2,
    )


def by_column(keep_one, came_one, keep_two, came_two):
    rows, cols = keep_one.shape
    n = cols // BLK

    def body(k1, c1, k2, c2, out):
        for i in range(n):
            at = slice(i * BLK, (i + 1) * BLK)
            out[i, :, :BLK] = k1[:, at] + c1[:, at]
            out[i, :, BLK:] = k2[:, at] + c2[:, at]

    return call(body, arr(n, rows, 2 * BLK), keep_one, came_one, keep_two, came_two)


def contract(parts, beside):
    n, rows, cols = parts.shape
    width = beside.shape[1] // 2
    half = 3 * width // 2

    def body(ins, left, total, keep, send, terms):
        v = ins[0]
        for i in range(1, n):
            v = v + ins[i]
        total[...] = v
        one = halves(v[:, :BLK])
        two = halves(v[:, BLK:])
        terms[: 2 * width, :] = dot3(halves(left[...]), one, ((0,), (0,)))
        terms[2 * width :, :] = dot3(halves(left[:, width:]), two, ((0,), (0,)))
        k = lax.axis_index("k")
        keep[...] = terms[pl.ds(pl.multiple_of(k * half, half), half), :]
        send[...] = terms[pl.ds(pl.multiple_of((1 - k) * half, half), half), :]

    shapes = [arr(rows, cols)] + [arr(half, BLK)] * 2
    return call(body, shapes, parts, beside, scratch=[pltpu.VMEM((2 * half, BLK), F32)])


def in_columns(cols, wide, body):
    def step(i, carry):
        body(pl.ds(pl.multiple_of(i * wide, wide), wide))
        return carry

    lax.fori_loop(0, cols // wide, step, 0)


def grams(lower_one, lower_two):
    side = lower_one.shape[0]

    def body(one, two, g1, g2):
        def part(at):
            for ref, out in ((one, g1), (two, g2)):
                out[:, at] = dot3(halves(ref[...]), halves(ref[:, at]), ((0,), (0,)))

        in_columns(side, 256, part)

    return call(body, [arr(side, side)] * 2, lower_one, lower_two)


def finish(mine, other, gram_one, gram_two, upper):
    n, rows, cols = mine.shape
    side = upper.shape[0]
    half = rows * 4

    def body(own, far, g1, g2, u_ref, d1_ref, c_ref, d2_ref, terms):
        k = lax.axis_index("k")
        for ref, core in ((own, k), (far, 1 - k)):
            for x in range(4):
                at = pl.ds(pl.multiple_of(core * half + x * rows, rows), rows)
                for y in range(4):
                    terms[at, y * cols : (y + 1) * cols] = ref[4 * x + y]
        d1_ref[...] = g1[...] + terms[:side, :]
        c_ref[...] = terms[side : 2 * side, :].T

        def coupling(at):
            c_ref[:, at] = c_ref[:, at] - dot3(halves(d1_ref[...]), halves(u_ref[:, at]), ((1,), (0,)))

        def last(at):
            cross = halves(terms[side : 2 * side, :])
            d2_ref[:, at] = (
                g2[:, at]
                + terms[2 * side :, at]
                - dot3(cross, halves(u_ref[:, at]), ((1,), (0,)))
                - dot3(halves(u_ref[...]), halves(c_ref[:, at]), ((0,), (0,)))
            )

        in_columns(side, 256, coupling)
        in_columns(side, 256, last)

    return call(
        body,
        [arr(side, side)] * 3,
        mine,
        other,
        gram_one,
        gram_two,
        upper,
        scratch=[pltpu.VMEM((2 * half, side), F32)],
    )


def product(left, right):
    return jnp.dot(left, right, precision=lax.Precision.HIGHEST, preferred_element_type=F32)


def owners():
    pairs = []
    for n in range(256):
        column, j = n // 32, n % 32
        zeta, beyond, core = j // 8, (j % 8) // 2, j % 2
        turn = ((2, 0), (1, 3))[beyond // 2][core]
        x = (column // 2 + turn) % 4
        z = (2 * zeta + beyond % 2 - 2 + 4 * (column % 2)) % 8
        pairs.append((n, (x * 8 + z) * 8 + column))
    return pairs


def ring(v, steps):
    ups, downs = [v], [v]
    for s in range(1, steps + 1):
        ups.append(shifted(ups[-1], "z", 1))
        if s < steps:
            downs.append(shifted(downs[-1], "z", -1))
    return ups, downs


def at_z(d):
    return lambda b: (jnp.int32(b), lax.rem(lax.axis_index("z") + d + 8, 8))


def at_x(d, first):
    return lambda b: (lax.rem(lax.axis_index("x") + d + 4, 4), jnp.int32(first + b))


def local(inverse_pool, panel_one, panel_two, upper_two, lower_one, lower_two, list_one, list_two):
    span, width = panel_one.shape
    both, masked_one, masked_two, keep_one, keep_two = masks(list_one, list_two, panel_one, panel_two)
    moved_two = lax.ppermute(masked_two, ALL, owners())
    moved_one = lax.ppermute(masked_one, ALL, owners())
    tile_hi, tile_lo = split_tile(inverse_pool, span)
    moved_one, moved_two, tile_hi, tile_lo = lax.optimization_barrier((moved_one, moved_two, tile_hi, tile_lo))

    ups, downs = ring(moved_two, 4)
    strips = stacked(spread(moved_one, "x"), "x", 2)
    strips, ups[3], downs[2] = lax.optimization_barrier((strips, ups[3], downs[2]))
    upper, lower = stacked_halves([moved_two, *ups[1:], *downs[:0:-1]], "z")

    (beside,) = stacked(spread(both, "y"), "y", 1)
    gram_one, gram_two = grams(lower_one, lower_two)

    sides = [shifted(v, "x", d) for v in (upper, lower) for d in (1, -1)]
    chunks_one = [(s, i * width // 2, at_z(0)) for i, s in enumerate(strips)]
    ups, downs = list(strips), list(strips)
    for s in range(1, 5):
        for i in range(2):
            ups[i] = shifted(ups[i], "z", 1)
            if s < 4:
                downs[i] = shifted(downs[i], "z", -1)
        if s == 2:
            ups, downs, sides, beside, gram_one, gram_two = lax.optimization_barrier(
                (ups, downs, sides, beside, gram_one, gram_two)
            )
            upper_up, upper_down, lower_up, lower_down = sides
            upper_far, lower_far = shifted(upper_down, "x", -1), shifted(lower_up, "x", 1)
        for i in range(2):
            chunks_one.append((ups[i], i * width // 2, at_z(-s)))
            if s < 4:
                chunks_one.append((downs[i], i * width // 2, at_z(s)))

    chunks_two = [
        (v, 0, at_x(d, first))
        for v, d, first in (
            (upper, 0, 0),
            (lower, 0, 4),
            (upper_up, -1, 0),
            (lower_up, -1, 4),
            (upper_down, 1, 0),
            (lower_down, 1, 4),
            (upper_far, 2, 0),
            (lower_far, 2, 4),
        )
    ]

    keep1, send1 = multiply(tile_hi, tile_lo, chunks_one, width, span)
    came1 = crossed(send1, "k", 1)
    keep2, send2 = multiply(tile_hi, tile_lo, chunks_two, width, span)
    came2 = crossed(send2, "k", 1)
    parts = traded(by_column(keep1, came1, keep2, came2), "y")
    total, keep, send = contract(parts, beside)

    terms = keep + crossed(send, "k", 1)
    terms = jnp.sum(traded(terms.reshape(4, -1, BLK), "x"), axis=0)
    lines = traded(total.reshape(4, span, 2 * BLK), "y")
    for mask in (1, 2, 4):
        terms = terms + crossed(terms, "z", mask)
        if mask == 2:
            terms, lines = lax.optimization_barrier((terms, lines))
    mine = traded(jnp.broadcast_to(terms, (16, *terms.shape)), ("x", "y"))
    other = crossed(mine, "k", 1)
    first_diag, second_coupling, second_diag = finish(mine, other, gram_one, gram_two, upper_two)

    product_one = jnp.swapaxes(lines[:, :, :BLK], 0, 1).reshape(span, width)
    product_two = jnp.swapaxes(lines[:, :, BLK:], 0, 1).reshape(span, width)
    first_offdiag = -keep_one[:, :1] * product_one
    second_offdiag = -keep_two[:, :1] * (product(first_offdiag, upper_two) + product_two)
    return (first_offdiag, first_diag, second_offdiag, second_coupling, second_diag)


def solution(mesh):
    finer = Mesh(mesh.devices.reshape(4, 8, 4, 2), ALL)
    rows, columns = ("x", "z"), ("y", "k")
    placed = (P(rows, columns), P(ALL, None), P(ALL, None), P(), P(), P(), P(), P())
    return jax.shard_map(
        local,
        mesh=finer,
        in_specs=placed,
        out_specs=(P(ALL, None), P(), P(ALL, None), P(), P()),
        check_vma=False,
    )
```

```python
import jax
import jax.numpy as jnp
from jax import lax
from jax.experimental import pallas as pl
from jax.experimental.pallas import tpu as pltpu
from jax.sharding import Mesh
from jax.sharding import PartitionSpec as P


BLK = 128
LEAD = 2
SIZES = {"x": 4, "z": 8, "y": 4, "k": 2}
ALL = ("x", "z", "y", "k")
F32 = jnp.float32
BF16 = jnp.bfloat16


def call(body, out_shapes, *args, scratch=()):
    whole = pl.BlockSpec(memory_space=pltpu.VMEM)
    return pl.pallas_call(
        body,
        out_shape=out_shapes,
        in_specs=[whole] * len(args),
        out_specs=jax.tree.map(lambda _: whole, out_shapes),
        scratch_shapes=list(scratch),
    )(*args)


def arr(*shape, dtype=F32):
    return jax.ShapeDtypeStruct(shape, dtype)


def halves(v):
    hi = v.astype(BF16)
    return hi, (v - hi.astype(F32)).astype(BF16)


def dot3(a, b, dims):
    def one(l, r):
        return lax.dot_general(l, r, (dims, ((), ())), preferred_element_type=F32)

    return one(a[0], b[0]) + (one(a[0], b[1]) + one(a[1], b[0]))


def shifted(v, axis, by):
    n = SIZES[axis]
    return lax.ppermute(v, axis, [(i, (i + by) % n) for i in range(n)])


def crossed(v, axis, mask):
    return lax.ppermute(v, axis, [(i, i ^ mask) for i in range(SIZES[axis])])


def traded(v, axis):
    return lax.all_to_all(v, axis, split_axis=0, concat_axis=0, tiled=True)


def spread(v, axis):
    return [v] + [shifted(v, axis, d) for d in range(1, SIZES[axis])]


def place(axis, d, step):
    n = SIZES[axis]
    return pl.multiple_of(lax.rem(lax.axis_index(axis) + (n + d) % n, n) * step, step)


def masks(list_one, list_two, panel_one, panel_two):
    rows, cols = panel_one.shape

    def body(one_list, two_list, one, two, both, out1, out2, keep1, keep2):
        index = lax.axis_index("x")
        for axis in ("z", "y", "k"):
            index = index * SIZES[axis] + lax.axis_index(axis)
        for listing, panel, out, keep, at in ((one_list, one, out1, keep1, 0), (two_list, two, out2, keep2, cols)):
            row = lax.broadcasted_iota(jnp.int32, (rows, listing.shape[1]), 0) + index * rows
            hits = jnp.where(lax.shift_right_logical(row, 7) == listing[...], 1.0, 0.0).astype(F32)
            live = jnp.max(hits, axis=1, keepdims=True)
            keep[...] = jnp.broadcast_to(live, (rows, BLK))
            v = live * panel[...]
            out[...] = v
            both[:, at : at + cols] = v

    shapes = [arr(rows, 2 * cols)] + [arr(rows, cols)] * 2 + [arr(rows, BLK)] * 2
    return call(body, shapes, list_one[None], list_two[None], panel_one, panel_two)


def split_tile(tile, span):
    rows, cols = tile.shape
    n = rows // (2 * span)

    def body(a, hi, lo):
        k = lax.axis_index("k")
        for half, core in ((0, k), (1, 1 - k)):
            for b in range(n):
                v = a[pl.ds(pl.multiple_of((2 * b + core) * span, span), span), :]
                h, l = halves(v)
                at = half * (rows // 2) + b * span
                hi[at : at + span, :] = h
                lo[at : at + span, :] = l

    return call(body, [arr(rows, cols, dtype=BF16)] * 2, tile)


def stacked(pieces, axis, cuts):
    n = SIZES[axis]
    rows, cols = pieces[0].shape
    width = cols // cuts

    def body(*refs):
        for d in range(n):
            for c in range(cuts):
                at = pl.ds(place(axis, -d, rows), rows)
                refs[n + c][at, :] = refs[d][:, c * width : (c + 1) * width]

    return call(body, [arr(n * rows, width)] * cuts, *pieces)


def stacked_halves(pieces, axis):
    n = SIZES[axis]
    rows, cols = pieces[0].shape

    def body(*refs):
        whole = refs[-1]
        for d in range(n):
            whole[pl.ds(place(axis, -d, rows), rows), :] = refs[d][...]
        refs[n][...] = whole[: n * rows // 2]
        refs[n + 1][...] = whole[n * rows // 2 :]

    return call(body, [arr(n * rows // 2, cols)] * 2, *pieces, scratch=[pltpu.VMEM((n * rows, cols), F32)])


def spot(x, z):
    order = lax.rem(z + 10 - 4 * lax.axis_index("k"), 8)
    turn = lax.rem(x + 4 - lax.axis_index("y"), 4)
    side = jnp.where(turn == 0, 1, jnp.where(turn == 1, 4, jnp.where(turn == 2, 0, 5)))
    return lax.shift_right_logical(order, 1) * 8 + lax.rem(order, 2) * 2 + side


def multiply(tile_hi, tile_lo, chunks, cols, span):
    rows, depth = tile_hi.shape
    m = len(chunks)
    wide = 256

    def body(*refs):
        hi, lo = refs[0], refs[1]
        keep, send, b_hi, b_lo = refs[2 + m :]
        for ref, (_, column, at_of) in zip(refs[2 : 2 + m], chunks):
            for b in range(ref.shape[0] // span):
                h, l = halves(ref[b * span : (b + 1) * span, :])
                at = pl.ds(pl.multiple_of(spot(*at_of(b)) * span, span), span)
                b_hi[at, column : column + ref.shape[1]] = h
                b_lo[at, column : column + ref.shape[1]] = l

        def step(i, carry):
            at = pl.ds(pl.multiple_of(i * wide, wide), wide)
            v = dot3((hi[...], lo[...]), (b_hi[:, at], b_lo[:, at]), ((1,), (0,)))
            keep[:, at] = v[: rows // 2]
            send[:, at] = v[rows // 2 :]
            return carry

        lax.fori_loop(0, cols // wide, step, 0)

    return call(
        body,
        [arr(rows // 2, cols)] * 2,
        tile_hi,
        tile_lo,
        *[c[0] for c in chunks],
        scratch=[pltpu.VMEM((depth, cols), BF16)] * 2,
    )


def by_column(keep_one, came_one, keep_two, came_two):
    rows, cols = keep_one.shape
    n = cols // BLK

    def body(k1, c1, k2, c2, out):
        for i in range(n):
            at = slice(i * BLK, (i + 1) * BLK)
            out[i, :, :BLK] = k1[:, at] + c1[:, at]
            out[i, :, BLK:] = k2[:, at] + c2[:, at]

    return call(body, arr(n, rows, 2 * BLK), keep_one, came_one, keep_two, came_two)


def contract(parts, beside):
    n, rows, cols = parts.shape
    span, depth = beside[0].shape
    width = depth // 2
    half = 3 * width // 2

    def body(ins, *refs):
        total, keep, send, terms, left = refs[n:]
        for d in range(n):
            left[pl.ds(place("y", -d, span), span), :] = refs[d][...]
        v = ins[0]
        for i in range(1, n):
            v = v + ins[i]
        total[...] = v
        one = halves(v[:, :BLK])
        two = halves(v[:, BLK:])
        terms[: 2 * width, :] = dot3(halves(left[...]), one, ((0,), (0,)))
        terms[2 * width :, :] = dot3(halves(left[:, width:]), two, ((0,), (0,)))
        k = lax.axis_index("k")
        keep[...] = terms[pl.ds(pl.multiple_of(k * half, half), half), :]
        send[...] = terms[pl.ds(pl.multiple_of((1 - k) * half, half), half), :]

    shapes = [arr(rows, cols)] + [arr(half, BLK)] * 2
    return call(
        body, shapes, parts, *beside, scratch=[pltpu.VMEM((2 * half, BLK), F32), pltpu.VMEM((rows, depth), F32)]
    )


def in_columns(cols, wide, body):
    def step(i, carry):
        body(pl.ds(pl.multiple_of(i * wide, wide), wide))
        return carry

    lax.fori_loop(0, cols // wide, step, 0)


def gram(lower):
    side = lower.shape[0]

    def body(ref, out):
        whole = halves(ref[...])

        def part(at):
            out[:, at] = dot3(whole, halves(ref[:, at]), ((0,), (0,)))

        in_columns(side, 256, part)

    return call(body, arr(side, side), lower)


def finish(mine, other, gram_one, gram_two, upper):
    _, rows, cols = mine.shape
    side = upper.shape[0]
    half = rows * 4

    def body(own, far, g1, g2, u_ref, d1_ref, c_ref, d2_ref, terms):
        k = lax.axis_index("k")
        for ref, core in ((own, k), (far, 1 - k)):
            for x in range(4):
                at = pl.ds(pl.multiple_of(core * half + x * rows, rows), rows)
                for y in range(4):
                    terms[at, y * cols : (y + 1) * cols] = ref[4 * x + y]
        d1_ref[...] = g1[...] + terms[:side, :]
        c_ref[...] = terms[side : 2 * side, :].T

        def coupling(at):
            c_ref[:, at] = c_ref[:, at] - dot3(halves(d1_ref[...]), halves(u_ref[:, at]), ((1,), (0,)))

        def last(at):
            cross = halves(terms[side : 2 * side, :])
            d2_ref[:, at] = (
                g2[:, at]
                + terms[2 * side :, at]
                - dot3(cross, halves(u_ref[:, at]), ((1,), (0,)))
                - dot3(halves(u_ref[...]), halves(c_ref[:, at]), ((0,), (0,)))
            )

        in_columns(side, 256, coupling)
        in_columns(side, 256, last)

    return call(
        body,
        [arr(side, side)] * 3,
        mine,
        other,
        gram_one,
        gram_two,
        upper,
        scratch=[pltpu.VMEM((2 * half, side), F32)],
    )


def product(left, right):
    return jnp.dot(left, right, precision=lax.Precision.HIGHEST, preferred_element_type=F32)


def owners():
    pairs = []
    for n in range(256):
        column, j = n // 32, n % 32
        zeta, beyond, core = j // 8, (j % 8) // 2, j % 2
        turn = ((2, 0), (1, 3))[beyond // 2][core]
        x = (column // 2 + turn) % 4
        z = (2 * zeta + beyond % 2 - 2 + 4 * (column % 2)) % 8
        pairs.append((n, (x * 8 + z) * 8 + column))
    return pairs


def at_z(d):
    return lambda b: (jnp.int32(b), lax.rem(lax.axis_index("z") + d + 8, 8))


def at_x(d, first):
    return lambda b: (lax.rem(lax.axis_index("x") + d + 4, 4), jnp.int32(first + b))


def inverted(inverse_pool, panel_one, panel_two, upper_two, lower_one, lower_two, list_one, list_two):
    span, width = panel_one.shape
    both, masked_one, masked_two, keep_one, keep_two = masks(list_one, list_two, panel_one, panel_two)
    moved_two = lax.ppermute(masked_two, ALL, owners())
    moved_one = lax.ppermute(masked_one, ALL, owners())
    tile_hi, tile_lo = split_tile(inverse_pool, span)
    beside = spread(both, "y")
    moved_one, moved_two, tile_hi, tile_lo, beside = lax.optimization_barrier(
        (moved_one, moved_two, tile_hi, tile_lo, beside)
    )

    fans = spread(moved_one, "x")
    ups, downs = [moved_two], [moved_two]
    for s in range(1, 5):
        ups.append(shifted(ups[-1], "z", 1))
        if s < 4:
            downs.append(shifted(downs[-1], "z", -1))
        if s == LEAD:
            fans, ups, downs = lax.optimization_barrier((fans, ups, downs))
    (strip,) = stacked(fans, "x", 1)
    upper, lower = stacked_halves([moved_two, *ups[1:], *downs[:0:-1]], "z")
    sides = []
    for v in (upper, lower):
        for d in (1, -1):
            sides.append(shifted(v, "x", d))
    upper_up, upper_down, lower_up, lower_down = sides
    upper_far = shifted(upper_down, "x", -1)
    lower_far = shifted(lower_up, "x", 1)

    chunks_one = [(strip, 0, at_z(0))]
    up = down = strip
    for s in range(1, 5):
        up = shifted(up, "z", 1)
        chunks_one.append((up, 0, at_z(-s)))
        if s < 4:
            down = shifted(down, "z", -1)
            chunks_one.append((down, 0, at_z(s)))
    chunks_two = [
        (v, 0, at_x(d, first))
        for v, d, first in (
            (upper, 0, 0),
            (lower, 0, 4),
            (upper_up, -1, 0),
            (lower_up, -1, 4),
            (upper_down, 1, 0),
            (lower_down, 1, 4),
            (upper_far, 2, 0),
            (lower_far, 2, 4),
        )
    ]

    keep1, send1 = multiply(tile_hi, tile_lo, chunks_one, width, span)
    came1 = crossed(send1, "k", 1)
    keep2, send2 = multiply(tile_hi, tile_lo, chunks_two, width, span)
    came2 = crossed(send2, "k", 1)
    parts = traded(by_column(keep1, came1, keep2, came2), "y")
    total, keep, send = contract(parts, beside)

    terms = keep + crossed(send, "k", 1)
    terms = jnp.sum(traded(terms.reshape(4, -1, BLK), "x"), axis=0)
    lines = traded(total.reshape(4, span, 2 * BLK), "y")
    for mask in (1, 2, 4):
        terms = terms + crossed(terms, "z", mask)
        if mask == 1:
            terms, gram_one = lax.optimization_barrier((terms, gram(lower_one)))
        if mask == 2:
            terms, lines, gram_two = lax.optimization_barrier((terms, lines, gram(lower_two)))
    mine = traded(jnp.broadcast_to(terms, (16, *terms.shape)), ("x", "y"))
    other = crossed(mine, "k", 1)
    first_diag, second_coupling, second_diag = finish(mine, other, gram_one, gram_two, upper_two)

    product_one = jnp.swapaxes(lines[:, :, :BLK], 0, 1).reshape(span, width)
    product_two = jnp.swapaxes(lines[:, :, BLK:], 0, 1).reshape(span, width)
    first_offdiag = -keep_one[:, :1] * product_one
    second_offdiag = -keep_two[:, :1] * (product(first_offdiag, upper_two) + product_two)
    return (first_offdiag, first_diag, second_offdiag, second_coupling, second_diag)


def solution(mesh):
    finer = Mesh(mesh.devices.reshape(4, 8, 4, 2), ALL)
    rows, columns = ("x", "z"), ("y", "k")
    placed = (P(rows, columns), P(ALL, None), P(ALL, None), P(), P(), P(), P(), P())
    return jax.shard_map(
        inverted,
        mesh=finer,
        in_specs=placed,
        out_specs=(P(ALL, None), P(), P(ALL, None), P(), P()),
        check_vma=False,
    )
```

```python
import jax
import jax.numpy as jnp
from jax import lax
from jax.experimental import pallas as pl
from jax.experimental.pallas import tpu as pltpu
from jax.sharding import Mesh
from jax.sharding import PartitionSpec as P


BLK = 128
LEAD = 2
SIZES = {"x": 4, "z": 8, "y": 4, "k": 2}
ALL = ("x", "z", "y", "k")
F32 = jnp.float32
BF16 = jnp.bfloat16


def call(body, out_shapes, *args, scratch=()):
    whole = pl.BlockSpec(memory_space=pltpu.VMEM)
    return pl.pallas_call(
        body,
        out_shape=out_shapes,
        in_specs=[whole] * len(args),
        out_specs=jax.tree.map(lambda _: whole, out_shapes),
        scratch_shapes=list(scratch),
    )(*args)


def arr(*shape, dtype=F32):
    return jax.ShapeDtypeStruct(shape, dtype)


def halves(v):
    hi = v.astype(BF16)
    return hi, (v - hi.astype(F32)).astype(BF16)


def dot3(a, b, dims):
    def one(l, r):
        return lax.dot_general(l, r, (dims, ((), ())), preferred_element_type=F32)

    return one(a[0], b[0]) + (one(a[0], b[1]) + one(a[1], b[0]))


def shifted(v, axis, by):
    n = SIZES[axis]
    return lax.ppermute(v, axis, [(i, (i + by) % n) for i in range(n)])


def crossed(v, axis, mask):
    return lax.ppermute(v, axis, [(i, i ^ mask) for i in range(SIZES[axis])])


def traded(v, axis):
    return lax.all_to_all(v, axis, split_axis=0, concat_axis=0, tiled=True)


def spread(v, axis):
    return [v] + [shifted(v, axis, d) for d in range(1, SIZES[axis])]


def place(axis, d, step):
    n = SIZES[axis]
    return pl.multiple_of(lax.rem(lax.axis_index(axis) + (n + d) % n, n) * step, step)


def masks(list_one, list_two, panel_one, panel_two):
    rows, cols = panel_one.shape

    def body(one_list, two_list, one, two, both, out1, out2, keep1, keep2):
        index = lax.axis_index("x")
        for axis in ("z", "y", "k"):
            index = index * SIZES[axis] + lax.axis_index(axis)
        for listing, panel, out, keep, at in ((one_list, one, out1, keep1, 0), (two_list, two, out2, keep2, cols)):
            row = lax.broadcasted_iota(jnp.int32, (rows, listing.shape[1]), 0) + index * rows
            hits = jnp.where(lax.shift_right_logical(row, 7) == listing[...], 1.0, 0.0).astype(F32)
            live = jnp.max(hits, axis=1, keepdims=True)
            keep[...] = jnp.broadcast_to(live, (rows, BLK))
            v = live * panel[...]
            out[...] = v
            both[:, at : at + cols] = v

    shapes = [arr(rows, 2 * cols)] + [arr(rows, cols)] * 2 + [arr(rows, BLK)] * 2
    return call(body, shapes, list_one[None], list_two[None], panel_one, panel_two)


def split_tile(tile, span):
    rows, cols = tile.shape
    n = rows // (2 * span)

    def body(a, hi, lo):
        k = lax.axis_index("k")
        for half, core in ((0, k), (1, 1 - k)):
            for b in range(n):
                v = a[pl.ds(pl.multiple_of((2 * b + core) * span, span), span), :]
                h, l = halves(v)
                at = half * (rows // 2) + b * span
                hi[at : at + span, :] = h
                lo[at : at + span, :] = l

    return call(body, [arr(rows, cols, dtype=BF16)] * 2, tile)


def stacked(pieces, axis, cuts):
    n = SIZES[axis]
    rows, cols = pieces[0].shape
    width = cols // cuts

    def body(*refs):
        for d in range(n):
            for c in range(cuts):
                at = pl.ds(place(axis, -d, rows), rows)
                refs[n + c][at, :] = refs[d][:, c * width : (c + 1) * width]

    return call(body, [arr(n * rows, width)] * cuts, *pieces)


def stacked_halves(pieces, axis):
    n = SIZES[axis]
    rows, cols = pieces[0].shape

    def body(*refs):
        whole = refs[-1]
        for d in range(n):
            whole[pl.ds(place(axis, -d, rows), rows), :] = refs[d][...]
        refs[n][...] = whole[: n * rows // 2]
        refs[n + 1][...] = whole[n * rows // 2 :]

    return call(body, [arr(n * rows // 2, cols)] * 2, *pieces, scratch=[pltpu.VMEM((n * rows, cols), F32)])


def spot(x, z):
    order = lax.rem(z + 10 - 4 * lax.axis_index("k"), 8)
    turn = lax.rem(x + 4 - lax.axis_index("y"), 4)
    side = jnp.where(turn == 0, 1, jnp.where(turn == 1, 4, jnp.where(turn == 2, 0, 5)))
    return lax.shift_right_logical(order, 1) * 8 + lax.rem(order, 2) * 2 + side


def multiply(tile_hi, tile_lo, chunks, cols, span):
    rows, depth = tile_hi.shape
    m = len(chunks)
    wide = 256

    def body(*refs):
        hi, lo = refs[0], refs[1]
        keep, send, b_hi, b_lo = refs[2 + m :]
        for ref, (_, column, at_of) in zip(refs[2 : 2 + m], chunks):
            for b in range(ref.shape[0] // span):
                h, l = halves(ref[b * span : (b + 1) * span, :])
                at = pl.ds(pl.multiple_of(spot(*at_of(b)) * span, span), span)
                b_hi[at, column : column + ref.shape[1]] = h
                b_lo[at, column : column + ref.shape[1]] = l

        def step(i, carry):
            at = pl.ds(pl.multiple_of(i * wide, wide), wide)
            v = dot3((hi[...], lo[...]), (b_hi[:, at], b_lo[:, at]), ((1,), (0,)))
            keep[:, at] = v[: rows // 2]
            send[:, at] = v[rows // 2 :]
            return carry

        lax.fori_loop(0, cols // wide, step, 0)

    return call(
        body,
        [arr(rows // 2, cols)] * 2,
        tile_hi,
        tile_lo,
        *[c[0] for c in chunks],
        scratch=[pltpu.VMEM((depth, cols), BF16)] * 2,
    )


def by_column(keep, came):
    rows, cols = keep.shape
    n = cols // BLK

    def body(own, far, out):
        for i in range(n):
            at = slice(i * BLK, (i + 1) * BLK)
            out[i] = own[:, at] + far[:, at]

    return call(body, arr(n, rows, BLK), keep, came)


def contract_two(parts, beside):
    n, rows, cols = parts.shape
    span, depth = beside[0].shape
    width = depth // 2

    def body(ins, *refs):
        total, left, terms = refs[n:]
        for d in range(n):
            left[pl.ds(place("y", -d, span), span), :] = refs[d][...]
        v = ins[0]
        for i in range(1, n):
            v = v + ins[i]
        total[...] = v
        terms[...] = dot3(halves(left[:, width:]), halves(v), ((0,), (0,)))

    return call(body, [arr(rows, cols), arr(rows, depth), arr(width, cols)], parts, *beside)


def contract_one(parts, left, total_two, terms_two):
    n, rows, cols = parts.shape
    width = terms_two.shape[0]
    half = 3 * width // 2

    def body(ins, left_ref, other, third, total, keep, send, terms):
        v = ins[0]
        for i in range(1, n):
            v = v + ins[i]
        total[:, :cols] = v
        total[:, cols:] = other[...]
        terms[: 2 * width, :] = dot3(halves(left_ref[...]), halves(v), ((0,), (0,)))
        terms[2 * width :, :] = third[...]
        k = lax.axis_index("k")
        keep[...] = terms[pl.ds(pl.multiple_of(k * half, half), half), :]
        send[...] = terms[pl.ds(pl.multiple_of((1 - k) * half, half), half), :]

    shapes = [arr(rows, 2 * cols)] + [arr(half, cols)] * 2
    return call(body, shapes, parts, left, total_two, terms_two, scratch=[pltpu.VMEM((2 * half, cols), F32)])


def in_columns(cols, wide, body):
    def step(i, carry):
        body(pl.ds(pl.multiple_of(i * wide, wide), wide))
        return carry

    lax.fori_loop(0, cols // wide, step, 0)


def gram(lower):
    side = lower.shape[0]

    def body(ref, out):
        whole = halves(ref[...])

        def part(at):
            out[:, at] = dot3(whole, halves(ref[:, at]), ((0,), (0,)))

        in_columns(side, 256, part)

    return call(body, arr(side, side), lower)


def finish(mine, other, gram_one, gram_two, upper):
    _, rows, cols = mine.shape
    side = upper.shape[0]
    half = rows * 4

    def body(own, far, g1, g2, u_ref, d1_ref, c_ref, d2_ref, terms):
        k = lax.axis_index("k")
        for ref, core in ((own, k), (far, 1 - k)):
            for x in range(4):
                at = pl.ds(pl.multiple_of(core * half + x * rows, rows), rows)
                for y in range(4):
                    terms[at, y * cols : (y + 1) * cols] = ref[4 * x + y]
        d1_ref[...] = g1[...] + terms[:side, :]
        c_ref[...] = terms[side : 2 * side, :].T

        def coupling(at):
            c_ref[:, at] = c_ref[:, at] - dot3(halves(d1_ref[...]), halves(u_ref[:, at]), ((1,), (0,)))

        def last(at):
            cross = halves(terms[side : 2 * side, :])
            d2_ref[:, at] = (
                g2[:, at]
                + terms[2 * side :, at]
                - dot3(cross, halves(u_ref[:, at]), ((1,), (0,)))
                - dot3(halves(u_ref[...]), halves(c_ref[:, at]), ((0,), (0,)))
            )

        in_columns(side, 256, coupling)
        in_columns(side, 256, last)

    return call(
        body,
        [arr(side, side)] * 3,
        mine,
        other,
        gram_one,
        gram_two,
        upper,
        scratch=[pltpu.VMEM((2 * half, side), F32)],
    )


def product(left, right):
    return jnp.dot(left, right, precision=lax.Precision.HIGHEST, preferred_element_type=F32)


def owners():
    pairs = []
    for n in range(256):
        column, j = n // 32, n % 32
        zeta, beyond, core = j // 8, (j % 8) // 2, j % 2
        turn = ((2, 0), (1, 3))[beyond // 2][core]
        x = (column // 2 + turn) % 4
        z = (2 * zeta + beyond % 2 - 2 + 4 * (column % 2)) % 8
        pairs.append((n, (x * 8 + z) * 8 + column))
    return pairs


def at_z(d):
    return lambda b: (jnp.int32(b), lax.rem(lax.axis_index("z") + d + 8, 8))


def at_x(d, first):
    return lambda b: (lax.rem(lax.axis_index("x") + d + 4, 4), jnp.int32(first + b))


def inverted(inverse_pool, panel_one, panel_two, upper_two, lower_one, lower_two, list_one, list_two):
    span, width = panel_one.shape
    both, masked_one, masked_two, keep_one, keep_two = masks(list_one, list_two, panel_one, panel_two)
    moved_two = lax.ppermute(masked_two, ALL, owners())
    moved_one = lax.ppermute(masked_one, ALL, owners())
    tile_hi, tile_lo = split_tile(inverse_pool, span)
    beside = [both]
    for d in range(1, 4):
        beside.append(shifted(both, "y", d))
    moved_one, moved_two, tile_hi, tile_lo, beside = lax.optimization_barrier(
        (moved_one, moved_two, tile_hi, tile_lo, beside)
    )

    fans = spread(moved_one, "x")
    ups, downs = [moved_two], [moved_two]
    for s in range(1, 5):
        ups.append(shifted(ups[-1], "z", 1))
        if s < 4:
            downs.append(shifted(downs[-1], "z", -1))
        if s == LEAD:
            fans, ups, downs = lax.optimization_barrier((fans, ups, downs))
    (strip,) = stacked(fans, "x", 1)
    upper, lower = stacked_halves([moved_two, *ups[1:], *downs[:0:-1]], "z")
    sides = []
    for v in (upper, lower):
        for d in (1, -1):
            sides.append(shifted(v, "x", d))
    upper_up, upper_down, lower_up, lower_down = sides
    upper_far = shifted(upper_down, "x", -1)
    lower_far = shifted(lower_up, "x", 1)
    upper_far, gram_one, gram_two = lax.optimization_barrier((upper_far, gram(lower_one), gram(lower_two)))

    chunks_one = [(strip, 0, at_z(0))]
    up = down = strip
    for s in range(1, 5):
        up = shifted(up, "z", 1)
        chunks_one.append((up, 0, at_z(-s)))
        if s < 4:
            down = shifted(down, "z", -1)
            chunks_one.append((down, 0, at_z(s)))
    chunks_two = [
        (v, 0, at_x(d, first))
        for v, d, first in (
            (upper, 0, 0),
            (lower, 0, 4),
            (upper_up, -1, 0),
            (lower_up, -1, 4),
            (upper_down, 1, 0),
            (lower_down, 1, 4),
            (upper_far, 2, 0),
            (lower_far, 2, 4),
        )
    ]

    keep2, send2 = multiply(tile_hi, tile_lo, chunks_two, width, span)
    parts = traded(by_column(keep2, crossed(send2, "k", 1)), "y")
    total_two, left, terms_two = contract_two(parts, beside)

    last, terms_two = lax.optimization_barrier((up, terms_two))
    chunks_one = [(last if v is up else v, c, p) for v, c, p in chunks_one]
    keep1, send1 = multiply(tile_hi, tile_lo, chunks_one, width, span)
    parts = traded(by_column(keep1, crossed(send1, "k", 1)), "y")
    total, keep, send = contract_one(parts, left, total_two, terms_two)

    terms = keep + crossed(send, "k", 1)
    terms = jnp.sum(traded(terms.reshape(4, -1, BLK), "x"), axis=0)
    lines = traded(total.reshape(4, span, 2 * BLK), "y")
    for mask in (1, 2, 4):
        terms = terms + crossed(terms, "z", mask)
        if mask == 2:
            terms, lines = lax.optimization_barrier((terms, lines))
    mine = traded(jnp.broadcast_to(terms, (16, *terms.shape)), ("x", "y"))
    other = crossed(mine, "k", 1)
    first_diag, second_coupling, second_diag = finish(mine, other, gram_one, gram_two, upper_two)

    product_one = jnp.swapaxes(lines[:, :, :BLK], 0, 1).reshape(span, width)
    product_two = jnp.swapaxes(lines[:, :, BLK:], 0, 1).reshape(span, width)
    first_offdiag = -keep_one[:, :1] * product_one
    second_offdiag = -keep_two[:, :1] * (product(first_offdiag, upper_two) + product_two)
    return (first_offdiag, first_diag, second_offdiag, second_coupling, second_diag)


def solution(mesh):
    finer = Mesh(mesh.devices.reshape(4, 8, 4, 2), ALL)
    rows, columns = ("x", "z"), ("y", "k")
    placed = (P(rows, columns), P(ALL, None), P(ALL, None), P(), P(), P(), P(), P())
    return jax.shard_map(
        inverted,
        mesh=finer,
        in_specs=placed,
        out_specs=(P(ALL, None), P(), P(ALL, None), P(), P()),
        check_vma=False,
    )
```

```python
import jax
import jax.numpy as jnp
from jax import lax
from jax.experimental import pallas as pl
from jax.experimental.pallas import tpu as pltpu
from jax.sharding import Mesh
from jax.sharding import PartitionSpec as P


BLK = 128
LEAD = 2
SIZES = {"x": 4, "z": 8, "y": 4, "k": 2}
ALL = ("x", "z", "y", "k")
F32 = jnp.float32
BF16 = jnp.bfloat16


def call(body, out_shapes, *args, scratch=()):
    whole = pl.BlockSpec(memory_space=pltpu.VMEM)
    return pl.pallas_call(
        body,
        out_shape=out_shapes,
        in_specs=[whole] * len(args),
        out_specs=jax.tree.map(lambda _: whole, out_shapes),
        scratch_shapes=list(scratch),
    )(*args)


def arr(*shape, dtype=F32):
    return jax.ShapeDtypeStruct(shape, dtype)


def halves(v):
    hi = v.astype(BF16)
    return hi, (v - hi.astype(F32)).astype(BF16)


def dot3(a, b, dims):
    def one(l, r):
        return lax.dot_general(l, r, (dims, ((), ())), preferred_element_type=F32)

    return one(a[0], b[0]) + (one(a[0], b[1]) + one(a[1], b[0]))


def shifted(v, axis, by):
    n = SIZES[axis]
    return lax.ppermute(v, axis, [(i, (i + by) % n) for i in range(n)])


def crossed(v, axis, mask):
    return lax.ppermute(v, axis, [(i, i ^ mask) for i in range(SIZES[axis])])


def traded(v, axis):
    return lax.all_to_all(v, axis, split_axis=0, concat_axis=0, tiled=True)


def spread(v, axis):
    return [v] + [shifted(v, axis, d) for d in range(1, SIZES[axis])]


def place(axis, d, step):
    n = SIZES[axis]
    return pl.multiple_of(lax.rem(lax.axis_index(axis) + (n + d) % n, n) * step, step)


def live_at(listing, first, rows):
    row = lax.broadcasted_iota(jnp.int32, (rows, listing.shape[1]), 0) + first
    hits = jnp.where(lax.shift_right_logical(row, 7) == listing[...], 1.0, 0.0).astype(F32)
    return jnp.max(hits, axis=1, keepdims=True)


def masks(list_one, list_two, panel_one, panel_two):
    rows, cols = panel_one.shape

    def body(one_list, two_list, one, two, both, keep1, keep2):
        index = lax.axis_index("x")
        for axis in ("z", "y", "k"):
            index = index * SIZES[axis] + lax.axis_index(axis)
        for listing, panel, keep, at in ((one_list, one, keep1, 0), (two_list, two, keep2, cols)):
            live = live_at(listing, index * rows, rows)
            keep[...] = jnp.broadcast_to(live, (rows, BLK))
            both[:, at : at + cols] = live * panel[...]

    shapes = [arr(rows, 2 * cols), arr(rows, BLK), arr(rows, BLK)]
    return call(body, shapes, list_one[None], list_two[None], panel_one, panel_two)


def column_masks(list_one, list_two, depth):
    def body(one_list, two_list, live1, live2):
        first = (lax.axis_index("y") * 2 + lax.axis_index("k")) * depth
        for listing, out in ((one_list, live1), (two_list, live2)):
            def put(i, carry, listing=listing, out=out):
                at = pl.multiple_of(i * BLK, BLK)
                out[pl.ds(at, BLK), :] = jnp.broadcast_to(live_at(listing, first + at, BLK), (BLK, BLK))
                return carry

            lax.fori_loop(0, depth // BLK, put, 0)

    return call(body, [arr(depth, BLK)] * 2, list_one[None], list_two[None])


def split_tile(tile, span):
    rows, cols = tile.shape
    n = rows // (2 * span)

    def body(a, hi, lo):
        k = lax.axis_index("k")
        for half, core in ((0, k), (1, 1 - k)):
            for b in range(n):
                v = a[pl.ds(pl.multiple_of((2 * b + core) * span, span), span), :]
                h, l = halves(v)
                at = half * (rows // 2) + b * span
                hi[at : at + span, :] = h
                lo[at : at + span, :] = l

    return call(body, [arr(rows, cols, dtype=BF16)] * 2, tile)


def stacked(pieces, axis, cuts):
    n = SIZES[axis]
    rows, cols = pieces[0].shape
    width = cols // cuts

    def body(*refs):
        for d in range(n):
            for c in range(cuts):
                at = pl.ds(place(axis, -d, rows), rows)
                refs[n + c][at, :] = refs[d][:, c * width : (c + 1) * width]

    return call(body, [arr(n * rows, width)] * cuts, *pieces)


def stacked_halves(pieces, axis):
    n = SIZES[axis]
    rows, cols = pieces[0].shape

    def body(*refs):
        whole = refs[-1]
        for d in range(n):
            whole[pl.ds(place(axis, -d, rows), rows), :] = refs[d][...]
        refs[n][...] = whole[: n * rows // 2]
        refs[n + 1][...] = whole[n * rows // 2 :]

    return call(body, [arr(n * rows // 2, cols)] * 2, *pieces, scratch=[pltpu.VMEM((n * rows, cols), F32)])


def spot(x, z):
    order = lax.rem(z + 10 - 4 * lax.axis_index("k"), 8)
    turn = lax.rem(x + 4 - lax.axis_index("y"), 4)
    side = jnp.where(turn == 0, 1, jnp.where(turn == 1, 4, jnp.where(turn == 2, 0, 5)))
    return lax.shift_right_logical(order, 1) * 8 + lax.rem(order, 2) * 2 + side


def multiply(tile_hi, tile_lo, live, chunks, cols, span):
    rows, depth = tile_hi.shape
    m = len(chunks)
    wide = 256

    def body(*refs):
        hi, lo, kept = refs[:3]
        keep, send, b_hi, b_lo = refs[3 + m :]
        for ref, (_, at_of) in zip(refs[3 : 3 + m], chunks):
            def put(b, carry, ref=ref, at_of=at_of):
                at = pl.ds(pl.multiple_of(spot(*at_of(b)) * span, span), span)
                rows_at = pl.ds(pl.multiple_of(b * span, span), span)
                mask = kept[at, :]
                for c in range(0, cols, BLK):
                    h, l = halves(mask * ref[rows_at, c : c + BLK])
                    b_hi[at, c : c + BLK] = h
                    b_lo[at, c : c + BLK] = l
                return carry

            lax.fori_loop(0, ref.shape[0] // span, put, 0)

        def step(i, carry):
            at = pl.ds(pl.multiple_of(i * wide, wide), wide)
            v = dot3((hi[...], lo[...]), (b_hi[:, at], b_lo[:, at]), ((1,), (0,)))
            keep[:, at] = v[: rows // 2]
            send[:, at] = v[rows // 2 :]
            return carry

        lax.fori_loop(0, cols // wide, step, 0)

    return call(
        body,
        [arr(rows // 2, cols)] * 2,
        tile_hi,
        tile_lo,
        live,
        *[c[0] for c in chunks],
        scratch=[pltpu.VMEM((depth, cols), BF16)] * 2,
    )


def by_column(keep_one, came_one, keep_two, came_two):
    rows, _ = keep_one.shape
    half = rows // 2

    def body(k1, c1, k2, c2, own, plus, minus, upper, lower):
        for d, outs in ((0, ((own, 0, rows),)), (1, ((plus, 0, rows),)), (3, ((minus, 0, rows),)),
                        (2, ((upper, 0, half), (lower, half, half)))):
            at = pl.ds(place("y", d, BLK), BLK)
            for out, first, count in outs:
                r = pl.ds(first, count)
                out[:, :BLK] = k1[r, at] + c1[r, at]
                out[:, BLK:] = k2[r, at] + c2[r, at]

    shapes = [arr(rows, 2 * BLK)] * 3 + [arr(half, 2 * BLK)] * 2
    return call(body, shapes, keep_one, came_one, keep_two, came_two)


def relayed(plus, minus, from_minus, from_plus):
    rows, cols = plus.shape
    half = rows // 2

    def body(p, m, t, b, p_out, m_out):
        p_out[:half] = p[:half] + t[...]
        p_out[half:] = p[half:]
        m_out[:half] = m[:half]
        m_out[half:] = m[half:] + b[...]

    return call(body, [arr(rows, cols)] * 2, plus, minus, from_minus, from_plus)


def summed_over_y(keep_one, came_one, keep_two, came_two):
    own, plus, minus, upper, lower = by_column(keep_one, came_one, keep_two, came_two)
    plus, minus = relayed(plus, minus, shifted(upper, "y", 1), shifted(lower, "y", -1))
    return own, shifted(plus, "y", 1), shifted(minus, "y", -1)


def contract(parts, beside):
    rows, cols = parts[0].shape
    span, depth = beside[0].shape
    width = depth // 2
    half = 3 * width // 2

    def body(a, b, c, *refs):
        total, keep, send, terms, left = refs[4:]
        for d in range(4):
            left[pl.ds(place("y", -d, span), span), :] = refs[d][...]
        v = a[...] + (b[...] + c[...])
        total[...] = v
        one = halves(v[:, :BLK])
        two = halves(v[:, BLK:])
        terms[: 2 * width, :] = dot3(halves(left[...]), one, ((0,), (0,)))
        terms[2 * width :, :] = dot3(halves(left[:, width:]), two, ((0,), (0,)))
        k = lax.axis_index("k")
        keep[...] = terms[pl.ds(pl.multiple_of(k * half, half), half), :]
        send[...] = terms[pl.ds(pl.multiple_of((1 - k) * half, half), half), :]

    shapes = [arr(rows, cols)] + [arr(half, BLK)] * 2
    return call(
        body, shapes, *parts, *beside, scratch=[pltpu.VMEM((2 * half, BLK), F32), pltpu.VMEM((rows, depth), F32)]
    )


def in_columns(cols, wide, body):
    def step(i, carry):
        body(pl.ds(pl.multiple_of(i * wide, wide), wide))
        return carry

    lax.fori_loop(0, cols // wide, step, 0)


def grams(lower_one, lower_two):
    side = lower_one.shape[0]
    wide = 256

    def body(one, two, g1, g2, both, out):
        both[0] = one[...]
        both[1] = two[...]

        def step(i, carry):
            which = lax.shift_right_logical(i, 1)
            at = pl.ds(pl.multiple_of(lax.rem(i, 2) * wide, wide), wide)
            out[which, :, at] = dot3(halves(both[which]), halves(both[which, :, at]), ((0,), (0,)))
            return carry

        lax.fori_loop(0, 2 * side // wide, step, 0)
        g1[...] = out[0]
        g2[...] = out[1]

    scratch = [pltpu.VMEM((2, side, side), F32)] * 2
    return call(body, [arr(side, side)] * 2, lower_one, lower_two, scratch=scratch)


def finish(mine, other, gram_one, gram_two, upper):
    _, rows, cols = mine.shape
    side = upper.shape[0]
    half = rows * 4

    def body(own, far, g1, g2, u_ref, d1_ref, c_ref, d2_ref, terms):
        k = lax.axis_index("k")
        for ref, core in ((own, k), (far, 1 - k)):
            def put(x, carry, ref=ref, core=core):
                at = pl.ds(pl.multiple_of(core * half + x * rows, rows), rows)
                for y in range(4):
                    terms[at, y * cols : (y + 1) * cols] = ref[4 * x + y]
                return carry

            lax.fori_loop(0, 4, put, 0)
        d1_ref[...] = g1[...] + terms[:side, :]
        c_ref[...] = terms[side : 2 * side, :].T

        def coupling(at):
            c_ref[:, at] = c_ref[:, at] - dot3(halves(d1_ref[...]), halves(u_ref[:, at]), ((1,), (0,)))

        def last(at):
            cross = halves(terms[side : 2 * side, :])
            d2_ref[:, at] = (
                g2[:, at]
                + terms[2 * side :, at]
                - dot3(cross, halves(u_ref[:, at]), ((1,), (0,)))
                - dot3(halves(u_ref[...]), halves(c_ref[:, at]), ((0,), (0,)))
            )

        in_columns(side, 256, coupling)
        in_columns(side, 256, last)

    return call(
        body,
        [arr(side, side)] * 3,
        mine,
        other,
        gram_one,
        gram_two,
        upper,
        scratch=[pltpu.VMEM((2 * half, side), F32)],
    )


def product(left, right):
    return jnp.dot(left, right, precision=lax.Precision.HIGH, preferred_element_type=F32)


def owners():
    pairs = []
    for n in range(256):
        column, j = n // 32, n % 32
        zeta, beyond, core = j // 8, (j % 8) // 2, j % 2
        turn = ((2, 0), (1, 3))[beyond // 2][core]
        x = (column // 2 + turn) % 4
        z = (2 * zeta + beyond % 2 - 2 + 4 * (column % 2)) % 8
        pairs.append((n, (x * 8 + z) * 8 + column))
    return pairs


def at_z(d):
    return lambda b: (b, lax.rem(lax.axis_index("z") + d + 8, 8))


def at_x(d, first):
    return lambda b: (lax.rem(lax.axis_index("x") + d + 4, 4), first + b)


def inverted(inverse_pool, panel_one, panel_two, upper_two, lower_one, lower_two, list_one, list_two):
    span, width = panel_one.shape
    moved_two = lax.ppermute(panel_two, ALL, owners())
    moved_one = lax.ppermute(panel_one, ALL, owners())
    both, keep_one, keep_two = masks(list_one, list_two, panel_one, panel_two)
    tile_hi, tile_lo = split_tile(inverse_pool, span)
    live_one, live_two = column_masks(list_one, list_two, inverse_pool.shape[1])
    beside = [both]
    for d in range(1, 4):
        beside.append(shifted(both, "y", d))
    moved_one, moved_two, tile_hi, tile_lo, live_one, live_two = lax.optimization_barrier(
        (moved_one, moved_two, tile_hi, tile_lo, live_one, live_two)
    )

    fans = spread(moved_one, "x")
    ups, downs = [moved_two], [moved_two]
    for s in range(1, 5):
        ups.append(shifted(ups[-1], "z", 1))
        if s < 4:
            downs.append(shifted(downs[-1], "z", -1))
        if s == LEAD:
            fans, ups, downs = lax.optimization_barrier((fans, ups, downs))
    (strip,) = stacked(fans, "x", 1)
    upper, lower = stacked_halves([moved_two, *ups[1:], *downs[:0:-1]], "z")
    sides = []
    for v in (upper, lower):
        for d in (1, -1):
            sides.append(shifted(v, "x", d))
    upper_up, upper_down, lower_up, lower_down = sides
    upper_far = shifted(upper_down, "x", -1)
    lower_far = shifted(lower_up, "x", 1)

    chunks_one = [(strip, at_z(0))]
    up = down = strip
    for s in range(1, 5):
        up = shifted(up, "z", 1)
        chunks_one.append((up, at_z(-s)))
        if s < 4:
            down = shifted(down, "z", -1)
            chunks_one.append((down, at_z(s)))
    chunks_two = [
        (v, at_x(d, first))
        for v, d, first in (
            (upper, 0, 0),
            (lower, 0, 4),
            (upper_up, -1, 0),
            (lower_up, -1, 4),
            (upper_down, 1, 0),
            (lower_down, 1, 4),
            (upper_far, 2, 0),
            (lower_far, 2, 4),
        )
    ]

    keep1, send1 = multiply(tile_hi, tile_lo, live_one, chunks_one, width, span)
    came1 = crossed(send1, "k", 1)
    keep2, send2 = multiply(tile_hi, tile_lo, live_two, chunks_two, width, span)
    came2 = crossed(send2, "k", 1)
    parts = summed_over_y(keep1, came1, keep2, came2)
    total, keep, send = contract(parts, beside)

    terms = keep + crossed(send, "k", 1)
    terms = jnp.sum(traded(terms.reshape(4, -1, BLK), "x"), axis=0)
    lines = traded(total.reshape(4, span, 2 * BLK), "y")
    for mask in (1, 2, 4):
        terms = terms + crossed(terms, "z", mask)
        if mask == 1:
            gram_one, gram_two = grams(lower_one, lower_two)
            terms, gram_one = lax.optimization_barrier((terms, gram_one))
        if mask == 2:
            terms, lines = lax.optimization_barrier((terms, lines))
    mine = traded(jnp.broadcast_to(terms, (16, *terms.shape)), ("x", "y"))
    other = crossed(mine, "k", 1)
    first_diag, second_coupling, second_diag = finish(mine, other, gram_one, gram_two, upper_two)

    product_one = jnp.swapaxes(lines[:, :, :BLK], 0, 1).reshape(span, width)
    product_two = jnp.swapaxes(lines[:, :, BLK:], 0, 1).reshape(span, width)
    first_offdiag = -keep_one[:, :1] * product_one
    second_offdiag = -keep_two[:, :1] * (product(first_offdiag, upper_two) + product_two)
    return (first_offdiag, first_diag, second_offdiag, second_coupling, second_diag)


def solution(mesh):
    finer = Mesh(mesh.devices.reshape(4, 8, 4, 2), ALL)
    rows, columns = ("x", "z"), ("y", "k")
    placed = (P(rows, columns), P(ALL, None), P(ALL, None), P(), P(), P(), P(), P())
    return jax.shard_map(
        inverted,
        mesh=finer,
        in_specs=placed,
        out_specs=(P(ALL, None), P(), P(ALL, None), P(), P()),
        check_vma=False,
    )
```

```python
import jax
import jax.numpy as jnp
from jax import lax
from jax.experimental import pallas as pl
from jax.experimental.pallas import tpu as pltpu
from jax.sharding import Mesh
from jax.sharding import PartitionSpec as P


BLK = 128
LEAD = 2
SIZES = {"x": 4, "z": 8, "y": 4, "k": 2}
ALL = ("x", "z", "y", "k")
F32 = jnp.float32
BF16 = jnp.bfloat16


def call(body, out_shapes, *args, scratch=()):
    whole = pl.BlockSpec(memory_space=pltpu.VMEM)
    return pl.pallas_call(
        body,
        out_shape=out_shapes,
        in_specs=[whole] * len(args),
        out_specs=jax.tree.map(lambda _: whole, out_shapes),
        scratch_shapes=list(scratch),
    )(*args)


def arr(*shape, dtype=F32):
    return jax.ShapeDtypeStruct(shape, dtype)


def halves(v):
    hi = v.astype(BF16)
    return hi, (v - hi.astype(F32)).astype(BF16)


def dot3(a, b, dims):
    def one(l, r):
        return lax.dot_general(l, r, (dims, ((), ())), preferred_element_type=F32)

    return one(a[0], b[0]) + (one(a[0], b[1]) + one(a[1], b[0]))


def shifted(v, axis, by):
    n = SIZES[axis]
    return lax.ppermute(v, axis, [(i, (i + by) % n) for i in range(n)])


def crossed(v, axis, mask):
    return lax.ppermute(v, axis, [(i, i ^ mask) for i in range(SIZES[axis])])


def traded(v, axis):
    return lax.all_to_all(v, axis, split_axis=0, concat_axis=0, tiled=True)


def spread(v, axis):
    return [v] + [shifted(v, axis, d) for d in range(1, SIZES[axis])]


def place(axis, d, step):
    n = SIZES[axis]
    return pl.multiple_of(lax.rem(lax.axis_index(axis) + (n + d) % n, n) * step, step)


def masks(list_one, list_two, panel_one, panel_two):
    rows, cols = panel_one.shape

    def body(one_list, two_list, one, two, both, out1, out2, keep1, keep2):
        index = lax.axis_index("x")
        for axis in ("z", "y", "k"):
            index = index * SIZES[axis] + lax.axis_index(axis)
        for listing, panel, out, keep, at in ((one_list, one, out1, keep1, 0), (two_list, two, out2, keep2, cols)):
            row = lax.broadcasted_iota(jnp.int32, (rows, listing.shape[1]), 0) + index * rows
            hits = jnp.where(lax.shift_right_logical(row, 7) == listing[...], 1.0, 0.0).astype(F32)
            live = jnp.max(hits, axis=1, keepdims=True)
            keep[...] = jnp.broadcast_to(live, (rows, BLK))
            v = live * panel[...]
            out[...] = v
            both[:, at : at + cols] = v

    shapes = [arr(rows, 2 * cols)] + [arr(rows, cols)] * 2 + [arr(rows, BLK)] * 2
    return call(body, shapes, list_one[None], list_two[None], panel_one, panel_two)


def split_tile(tile, span):
    rows, cols = tile.shape
    n = rows // (2 * span)

    def body(a, hi, lo):
        k = lax.axis_index("k")
        for half, core in ((0, k), (1, 1 - k)):
            for b in range(n):
                v = a[pl.ds(pl.multiple_of((2 * b + core) * span, span), span), :]
                h, l = halves(v)
                at = half * (rows // 2) + b * span
                hi[at : at + span, :] = h
                lo[at : at + span, :] = l

    return call(body, [arr(rows, cols, dtype=BF16)] * 2, tile)


def stacked(pieces, axis, cuts):
    n = SIZES[axis]
    rows, cols = pieces[0].shape
    width = cols // cuts

    def body(*refs):
        for d in range(n):
            for c in range(cuts):
                at = pl.ds(place(axis, -d, rows), rows)
                refs[n + c][at, :] = refs[d][:, c * width : (c + 1) * width]

    return call(body, [arr(n * rows, width)] * cuts, *pieces)


def stacked_halves(pieces, axis):
    n = SIZES[axis]
    rows, cols = pieces[0].shape

    def body(*refs):
        whole = refs[-1]
        for d in range(n):
            whole[pl.ds(place(axis, -d, rows), rows), :] = refs[d][...]
        refs[n][...] = whole[: n * rows // 2]
        refs[n + 1][...] = whole[n * rows // 2 :]

    return call(body, [arr(n * rows // 2, cols)] * 2, *pieces, scratch=[pltpu.VMEM((n * rows, cols), F32)])


def spot(x, z):
    order = lax.rem(z + 10 - 4 * lax.axis_index("k"), 8)
    turn = lax.rem(x + 4 - lax.axis_index("y"), 4)
    side = jnp.where(turn == 0, 1, jnp.where(turn == 1, 4, jnp.where(turn == 2, 0, 5)))
    return lax.shift_right_logical(order, 1) * 8 + lax.rem(order, 2) * 2 + side


def multiply(tile_hi, tile_lo, chunks, cols, span):
    rows, depth = tile_hi.shape
    m = len(chunks)
    wide = 256

    def body(*refs):
        hi, lo = refs[0], refs[1]
        keep, send, b_hi, b_lo = refs[2 + m :]
        for ref, (_, column, at_of) in zip(refs[2 : 2 + m], chunks):
            for b in range(ref.shape[0] // span):
                h, l = halves(ref[b * span : (b + 1) * span, :])
                at = pl.ds(pl.multiple_of(spot(*at_of(b)) * span, span), span)
                b_hi[at, column : column + ref.shape[1]] = h
                b_lo[at, column : column + ref.shape[1]] = l

        def step(i, carry):
            at = pl.ds(pl.multiple_of(i * wide, wide), wide)
            v = dot3((hi[...], lo[...]), (b_hi[:, at], b_lo[:, at]), ((1,), (0,)))
            keep[:, at] = v[: rows // 2]
            send[:, at] = v[rows // 2 :]
            return carry

        lax.fori_loop(0, cols // wide, step, 0)

    return call(
        body,
        [arr(rows // 2, cols)] * 2,
        tile_hi,
        tile_lo,
        *[c[0] for c in chunks],
        scratch=[pltpu.VMEM((depth, cols), BF16)] * 2,
    )


def by_column(keep_one, came_one, keep_two, came_two):
    rows, _ = keep_one.shape
    half = rows // 2

    def body(k1, c1, k2, c2, own, plus, minus, upper, lower):
        for d, outs in ((0, ((own, 0, rows),)), (1, ((plus, 0, rows),)), (3, ((minus, 0, rows),)),
                        (2, ((upper, 0, half), (lower, half, half)))):
            at = pl.ds(place("y", d, BLK), BLK)
            for out, first, count in outs:
                r = pl.ds(first, count)
                out[:, :BLK] = k1[r, at] + c1[r, at]
                out[:, BLK:] = k2[r, at] + c2[r, at]

    shapes = [arr(rows, 2 * BLK)] * 3 + [arr(half, 2 * BLK)] * 2
    return call(body, shapes, keep_one, came_one, keep_two, came_two)


def relayed(plus, minus, from_minus, from_plus):
    rows, cols = plus.shape
    half = rows // 2

    def body(p, m, t, b, p_out, m_out):
        p_out[:half] = p[:half] + t[...]
        p_out[half:] = p[half:]
        m_out[:half] = m[:half]
        m_out[half:] = m[half:] + b[...]

    return call(body, [arr(rows, cols)] * 2, plus, minus, from_minus, from_plus)


def summed_over_y(keep_one, came_one, keep_two, came_two):
    own, plus, minus, upper, lower = by_column(keep_one, came_one, keep_two, came_two)
    plus, minus = relayed(plus, minus, shifted(upper, "y", 1), shifted(lower, "y", -1))
    return own, shifted(plus, "y", 1), shifted(minus, "y", -1)


def contract(parts, beside):
    rows, cols = parts[0].shape
    span, depth = beside[0].shape
    width = depth // 2
    half = 3 * width // 2

    def body(a, b, c, *refs):
        total, keep, send, terms, left = refs[4:]
        for d in range(4):
            left[pl.ds(place("y", -d, span), span), :] = refs[d][...]
        v = a[...] + (b[...] + c[...])
        total[...] = v
        one = halves(v[:, :BLK])
        two = halves(v[:, BLK:])
        terms[: 2 * width, :] = dot3(halves(left[...]), one, ((0,), (0,)))
        terms[2 * width :, :] = dot3(halves(left[:, width:]), two, ((0,), (0,)))
        k = lax.axis_index("k")
        keep[...] = terms[pl.ds(pl.multiple_of(k * half, half), half), :]
        send[...] = terms[pl.ds(pl.multiple_of((1 - k) * half, half), half), :]

    shapes = [arr(rows, cols)] + [arr(half, BLK)] * 2
    return call(
        body, shapes, *parts, *beside, scratch=[pltpu.VMEM((2 * half, BLK), F32), pltpu.VMEM((rows, depth), F32)]
    )


def in_columns(cols, wide, body):
    def step(i, carry):
        body(pl.ds(pl.multiple_of(i * wide, wide), wide))
        return carry

    lax.fori_loop(0, cols // wide, step, 0)


def grams(lower_one, lower_two):
    side = lower_one.shape[0]
    wide = 256

    def body(one, two, g1, g2, both, out):
        both[0] = one[...]
        both[1] = two[...]

        def step(i, carry):
            which = lax.shift_right_logical(i, 1)
            at = pl.ds(pl.multiple_of(lax.rem(i, 2) * wide, wide), wide)
            out[which, :, at] = dot3(halves(both[which]), halves(both[which, :, at]), ((0,), (0,)))
            return carry

        lax.fori_loop(0, 2 * side // wide, step, 0)
        g1[...] = out[0]
        g2[...] = out[1]

    scratch = [pltpu.VMEM((2, side, side), F32)] * 2
    return call(body, [arr(side, side)] * 2, lower_one, lower_two, scratch=scratch)


def finish(mine, other, gram_one, gram_two, upper):
    _, rows, cols = mine.shape
    side = upper.shape[0]
    half = rows * 4

    def body(own, far, g1, g2, u_ref, d1_ref, c_ref, d2_ref, terms):
        k = lax.axis_index("k")
        for ref, core in ((own, k), (far, 1 - k)):
            def put(x, carry, ref=ref, core=core):
                at = pl.ds(pl.multiple_of(core * half + x * rows, rows), rows)
                for y in range(4):
                    terms[at, y * cols : (y + 1) * cols] = ref[4 * x + y]
                return carry

            lax.fori_loop(0, 4, put, 0)
        d1_ref[...] = g1[...] + terms[:side, :]
        c_ref[...] = terms[side : 2 * side, :].T

        def coupling(at):
            c_ref[:, at] = c_ref[:, at] - dot3(halves(d1_ref[...]), halves(u_ref[:, at]), ((1,), (0,)))

        def last(at):
            cross = halves(terms[side : 2 * side, :])
            d2_ref[:, at] = (
                g2[:, at]
                + terms[2 * side :, at]
                - dot3(cross, halves(u_ref[:, at]), ((1,), (0,)))
                - dot3(halves(u_ref[...]), halves(c_ref[:, at]), ((0,), (0,)))
            )

        in_columns(side, 256, coupling)
        in_columns(side, 256, last)

    return call(
        body,
        [arr(side, side)] * 3,
        mine,
        other,
        gram_one,
        gram_two,
        upper,
        scratch=[pltpu.VMEM((2 * half, side), F32)],
    )


def product(left, right):
    return jnp.dot(left, right, precision=lax.Precision.HIGH, preferred_element_type=F32)


def owners():
    pairs = []
    for n in range(256):
        column, j = n // 32, n % 32
        zeta, beyond, core = j // 8, (j % 8) // 2, j % 2
        turn = ((2, 0), (1, 3))[beyond // 2][core]
        x = (column // 2 + turn) % 4
        z = (2 * zeta + beyond % 2 - 2 + 4 * (column % 2)) % 8
        pairs.append((n, (x * 8 + z) * 8 + column))
    return pairs


def at_z(d):
    return lambda b: (b, lax.rem(lax.axis_index("z") + d + 8, 8))


def at_x(d, first):
    return lambda b: (lax.rem(lax.axis_index("x") + d + 4, 4), first + b)


def inverted(inverse_pool, panel_one, panel_two, upper_two, lower_one, lower_two, list_one, list_two):
    span, width = panel_one.shape
    both, masked_one, masked_two, keep_one, keep_two = masks(list_one, list_two, panel_one, panel_two)
    moved_two = lax.ppermute(masked_two, ALL, owners())
    moved_one = lax.ppermute(masked_one, ALL, owners())
    tile_hi, tile_lo = split_tile(inverse_pool, span)
    beside = spread(both, "y")
    moved_one, moved_two, tile_hi, tile_lo, beside = lax.optimization_barrier(
        (moved_one, moved_two, tile_hi, tile_lo, beside)
    )

    fans = spread(moved_one, "x")
    ups, downs = [moved_two], [moved_two]
    for s in range(1, 5):
        ups.append(shifted(ups[-1], "z", 1))
        if s < 4:
            downs.append(shifted(downs[-1], "z", -1))
        if s == LEAD:
            fans, ups, downs = lax.optimization_barrier((fans, ups, downs))
    (strip,) = stacked(fans, "x", 1)
    upper, lower = stacked_halves([moved_two, *ups[1:], *downs[:0:-1]], "z")
    sides = []
    for v in (upper, lower):
        for d in (1, -1):
            sides.append(shifted(v, "x", d))
    upper_up, upper_down, lower_up, lower_down = sides
    upper_far = shifted(upper_down, "x", -1)
    lower_far = shifted(lower_up, "x", 1)

    chunks_one = [(strip, 0, at_z(0))]
    up = down = strip
    for s in range(1, 5):
        up = shifted(up, "z", 1)
        chunks_one.append((up, 0, at_z(-s)))
        if s < 4:
            down = shifted(down, "z", -1)
            chunks_one.append((down, 0, at_z(s)))
    chunks_two = [
        (v, 0, at_x(d, first))
        for v, d, first in (
            (upper, 0, 0),
            (lower, 0, 4),
            (upper_up, -1, 0),
            (lower_up, -1, 4),
            (upper_down, 1, 0),
            (lower_down, 1, 4),
            (upper_far, 2, 0),
            (lower_far, 2, 4),
        )
    ]

    keep1, send1 = multiply(tile_hi, tile_lo, chunks_one, width, span)
    came1 = crossed(send1, "k", 1)
    keep2, send2 = multiply(tile_hi, tile_lo, chunks_two, width, span)
    came2 = crossed(send2, "k", 1)
    parts = summed_over_y(keep1, came1, keep2, came2)
    total, keep, send = contract(parts, beside)

    terms = keep + crossed(send, "k", 1)
    terms = jnp.sum(traded(terms.reshape(4, -1, BLK), "x"), axis=0)
    lines = traded(total.reshape(4, span, 2 * BLK), "y")
    for mask in (1, 2, 4):
        terms = terms + crossed(terms, "z", mask)
        if mask == 1:
            gram_one, gram_two = grams(lower_one, lower_two)
            terms, gram_one = lax.optimization_barrier((terms, gram_one))
        if mask == 2:
            terms, lines = lax.optimization_barrier((terms, lines))
    mine = traded(jnp.broadcast_to(terms, (16, *terms.shape)), ("x", "y"))
    other = crossed(mine, "k", 1)
    first_diag, second_coupling, second_diag = finish(mine, other, gram_one, gram_two, upper_two)

    product_one = jnp.swapaxes(lines[:, :, :BLK], 0, 1).reshape(span, width)
    product_two = jnp.swapaxes(lines[:, :, BLK:], 0, 1).reshape(span, width)
    first_offdiag = -keep_one[:, :1] * product_one
    second_offdiag = -keep_two[:, :1] * (product(first_offdiag, upper_two) + product_two)
    return (first_offdiag, first_diag, second_offdiag, second_coupling, second_diag)


def solution(mesh):
    finer = Mesh(mesh.devices.reshape(4, 8, 4, 2), ALL)
    rows, columns = ("x", "z"), ("y", "k")
    placed = (P(rows, columns), P(ALL, None), P(ALL, None), P(), P(), P(), P(), P())
    return jax.shard_map(
        inverted,
        mesh=finer,
        in_specs=placed,
        out_specs=(P(ALL, None), P(), P(ALL, None), P(), P()),
        check_vma=False,
    )
```
